32 devices in a mesh: dp: 8 (over z, x), tensor: 4 (over y, core).
Axes of the slice: x: 2, y: 2, z: 4, core: 2. Of those that a mesh axis runs over, the one named last changes fastest.
Arguments:
- patches: bfloat16 [16, 4, 512, 1024], P(None, 'tensor', 'dp'), may hold values from -6 to 6
- lengths: int32 [16], replicated, may hold values from 1024 to 2048, as said below
- deal: int32 [16], replicated, may hold values from 0 to 15, as said below
- attn_gain: float32 [1024], replicated, may hold values from 0.25 to 1.75
- w_query: bfloat16 [1024, 1024], P(None, 'tensor'), may hold values from -0.1875 to 0.1875
- w_key: bfloat16 [1024, 1024], P(None, 'tensor'), may hold values from -0.1875 to 0.1875
- w_value: bfloat16 [1024, 1024], P(None, 'tensor'), may hold values from -0.1875 to 0.1875
- w_out: bfloat16 [1024, 1024], P('tensor'), may hold values from -1.5 to 1.5
- ffn_gain: float32 [1024], replicated, may hold values from 0.25 to 1.75
- w_gate: bfloat16 [1024, 2816], P(None, 'tensor'), may hold values from -0.1875 to 0.1875
- w_up: bfloat16 [1024, 2816], P(None, 'tensor'), may hold values from -0.1875 to 0.1875
- w_down: bfloat16 [2816, 1024], P('tensor'), may hold values from -0.109375 to 0.109375
- cotangent: bfloat16 [16, 4, 512, 1024], P('dp', 'tensor'), may hold values from -6 to 6
Outputs:
- output: bfloat16 [16, 4, 512, 1024], P('dp', 'tensor')
- grad_patches: bfloat16 [16, 4, 512, 1024], P(None, 'tensor', 'dp')
- grad_attn_gain: float32 [1024], replicated
- grad_w_query: float32 [1024, 1024], P('dp', 'tensor')
- grad_w_key: float32 [1024, 1024], P('dp', 'tensor')
- grad_w_value: float32 [1024, 1024], P('dp', 'tensor')
- grad_w_out: float32 [1024, 1024], P('tensor', 'dp')
- grad_ffn_gain: float32 [1024], replicated
- grad_w_gate: float32 [1024, 2816], P('dp', 'tensor')
- grad_w_up: float32 [1024, 2816], P('dp', 'tensor')
- grad_w_down: float32 [2816, 1024], P('tensor', 'dp')
The draws below stay inside these ranges and needn't reach their ends.
Inputs may be any that keep to these rules, and one draw needn't show every extreme that they name: `lengths`: length of sequence s; positions from it on are padding, and one sequence has length 2048, one 1024. A permutation: sequence s goes to slot deal[s], which lies in data group deal[s] // 2.
All inputs are finite; a program needn't handle non-finite values.
Results may differ from the reference program's by a relative error of at most 0.02.
Values may be sent and summed in bfloat16 or wider, within the bound.
A program may use at most 256 MiB of HBM per device.

```python
import jax
import jax.numpy as jnp
from jax import lax

D = 1024
HEADS = 16
HEAD_DIM = 64
FF = 2816
SEQ_DEV = 2
LMAX = 2048
LMIN = 1024
SEQS = 16
TSPLIT = 4
QUARTER = 512
N_TENSOR = 4


def lengths_and_deal(key):
    folded = jax.random.fold_in(key, 17)
    first_key, second_key, third_key = jax.random.split(folded, 3)
    drawn_lengths = jax.random.randint(first_key, (SEQS,), LMIN, LMAX + 1)
    longest_at = jax.random.randint(second_key, (), 0, SEQS)
    drawn_lengths = drawn_lengths.at[longest_at].set(LMAX)
    drawn_lengths = drawn_lengths.at[(longest_at + 1) % SEQS].set(LMIN)
    ranked = jnp.argsort(-drawn_lengths, stable=True)
    group_count = SEQS // SEQ_DEV
    places = jnp.arange(SEQS)
    rounds = places // group_count
    within = places % group_count
    snake_group = jnp.where(rounds % 2 == 0, within, group_count - 1 - within)
    relabel = jax.random.permutation(third_key, group_count)
    slot_number = relabel[snake_group] * SEQ_DEV + rounds
    dealt_slots = jnp.zeros((SEQS,), jnp.int32).at[ranked].set(slot_number.astype(jnp.int32))
    return (drawn_lengths.astype(jnp.int32), dealt_slots)


def draw_lengths(key, part):
    return lengths_and_deal(key)[0]


def draw_deal(key, part):
    return lengths_and_deal(key)[1]


def level_of(own_key, extent, cuts, low, high):
    gain = 1.0
    for axis_at, shards_of in cuts:
        draws = jax.random.uniform(jax.random.fold_in(jax.random.fold_in(own_key, 6), axis_at), (shards_of,), jnp.float32, low / len(cuts), high / len(cuts))
        gain = gain * jnp.repeat(jnp.exp(draws), extent[axis_at] // shards_of).reshape((-1,) + (1,) * (len(extent) - 1 - axis_at))
    return gain


def normal_values(key, dims, width, limit, cuts=(), dtype=jnp.bfloat16):
    gain = level_of(key, dims, cuts, -0.22, 0.18) if cuts else 1.0
    values = jax.random.normal(key, dims, jnp.float32) * width * gain
    return jnp.minimum(jnp.maximum(values, -limit), limit).astype(dtype)


def setup_inputs(seed: int = 0) -> dict:
    arg_keys = jax.random.split(jax.random.key(seed), 14)
    return {
        "patches": normal_values(arg_keys[0], (SEQS, TSPLIT, QUARTER, D), 1.0, 6.0, ((1, 4), (2, 8))),
        "lengths": draw_lengths(jax.random.fold_in(arg_keys[13], 71), 0),
        "deal": draw_deal(jax.random.fold_in(arg_keys[13], 71), 0),
        "attn_gain": jnp.clip(1.0 + 0.15 * jax.random.normal(arg_keys[3], (D,), jnp.float32), 0.25, 1.75),
        "w_query": normal_values(arg_keys[4], (D, D), D ** -0.5, 0.1875, ((1, 4),)),
        "w_key": normal_values(arg_keys[5], (D, D), D ** -0.5, 0.1875, ((1, 4),)),
        "w_value": normal_values(arg_keys[6], (D, D), D ** -0.5, 0.1875, ((1, 4),)),
        "w_out": normal_values(arg_keys[7], (D, D), 16 ** -0.5, 1.5, ((0, 4),)),
        "ffn_gain": jnp.clip(1.0 + 0.15 * jax.random.normal(arg_keys[8], (D,), jnp.float32), 0.25, 1.75),
        "w_gate": normal_values(arg_keys[9], (D, FF), D ** -0.5, 0.1875, ((1, 4),)),
        "w_up": normal_values(arg_keys[10], (D, FF), D ** -0.5, 0.1875, ((1, 4),)),
        "w_down": normal_values(arg_keys[11], (FF, D), FF ** -0.5, 0.109375, ((0, 4),)),
        "cotangent": normal_values(arg_keys[12], (SEQS, TSPLIT, QUARTER, D), 1.0, 6.0, ((0, 8), (1, 4))),
    }


EPSILON = 1e-05
NEGATIVE = -1e+30
HIGHEST_PRECISION = lax.Precision.HIGHEST

@jax.custom_vjp
def low(v):
    return lax.optimization_barrier(v.astype(jnp.bfloat16)).astype(jnp.float32)

@jax.custom_vjp
def low_back(v):
    return v

def low_keep(v):
    return (low(v), None)

def low_pass(kept, grad):
    return (grad,)

def back_keep(v):
    return (v, None)

def back_low(kept, grad):
    return (low(grad),)
low.defvjp(low_keep, low_pass)
low_back.defvjp(back_keep, back_low)

def norm_rows(value_tensor, gain_vector):
    return value_tensor * lax.rsqrt(lax.optimization_barrier(jnp.mean(value_tensor * value_tensor, -1, keepdims=True)) + EPSILON) * gain_vector

def layer_one(params, patch_rows, length):
    attn_gain, w_query, w_key, w_value, w_out, ffn_gain, w_gate, w_up, w_down = params
    part_count = N_TENSOR
    shard_width = D // part_count
    hidden_part = FF // part_count
    heads_part = HEADS // part_count
    positions = jnp.arange(LMAX)
    live_rows = (positions < length).astype(jnp.float32)[:, None]

    def columns(weight_matrix, count):
        return weight_matrix.reshape(D, part_count, count).transpose(1, 0, 2)

    def heads_of(value_tensor):
        return value_tensor.reshape(part_count, LMAX, heads_part, HEAD_DIM).transpose(0, 2, 1, 3).reshape(HEADS, LMAX, HEAD_DIM)
    normed_attn = low(norm_rows(patch_rows, attn_gain))
    copies_attn = low_back(jnp.broadcast_to(normed_attn, (part_count, LMAX, D)))

    def project_heads(weight_matrix):
        projected = jnp.einsum('tld,tdk->tlk', copies_attn, columns(weight_matrix, shard_width), precision=HIGHEST_PRECISION)
        return heads_of(low_back(low(projected)))
    queries = project_heads(w_query)
    key_rows = project_heads(w_key)
    value_rows = project_heads(w_value)
    scores = low_back(jnp.einsum('hqd,hkd->hqk', queries, key_rows, precision=HIGHEST_PRECISION) * HEAD_DIM ** (-0.5))
    causal = positions[:, None] >= positions[None, :]
    scores = jnp.where(causal, scores, NEGATIVE)
    highest = lax.optimization_barrier(jnp.max(scores, -1, keepdims=True))
    log_total = highest + jnp.log(lax.optimization_barrier(jnp.sum(jnp.exp(scores - highest), -1, keepdims=True)))
    probabilities = low(jnp.exp(scores - log_total))
    mixed_rows = jnp.einsum('hqk,hkd->hqd', probabilities, value_rows, precision=HIGHEST_PRECISION)
    mixed_rows = mixed_rows.reshape(part_count, heads_part, LMAX, HEAD_DIM).transpose(0, 2, 1, 3).reshape(part_count, LMAX, shard_width)
    mixed_rows = low_back(low(mixed_rows))
    attn_parts = jnp.einsum('tlk,tkd->tld', mixed_rows, w_out.reshape(part_count, shard_width, D), precision=HIGHEST_PRECISION)
    attention = low_back(lax.optimization_barrier(jnp.sum(low(attn_parts), 0)))
    hidden = patch_rows + attention
    normed_ffn = low(norm_rows(hidden, ffn_gain))
    copies_ffn = low_back(jnp.broadcast_to(normed_ffn, (part_count, LMAX, D)))
    gate_pre = low_back(jnp.einsum('tld,tdf->tlf', copies_ffn, columns(w_gate, hidden_part), precision=HIGHEST_PRECISION))
    up_proj = low_back(jnp.einsum('tld,tdf->tlf', copies_ffn, columns(w_up, hidden_part), precision=HIGHEST_PRECISION))
    product = low(gate_pre / (1.0 + jnp.exp(-gate_pre)) * up_proj)
    ffn_parts = jnp.einsum('tlf,tfd->tld', product, w_down.reshape(part_count, hidden_part, D), precision=HIGHEST_PRECISION)
    feedforward = low_back(lax.optimization_barrier(jnp.sum(low(ffn_parts), 0)))
    return live_rows * (hidden + feedforward)

def reference(patches, lengths, deal, attn_gain, w_query, w_key, w_value, w_out, ffn_gain, w_gate, w_up, w_down, cotangent):
    seq_total = patches.shape[0]
    slot_owner = jnp.argsort(deal).astype(jnp.int32)
    own_lengths = lengths[slot_owner]
    patch_rows = patches.astype(jnp.float32).reshape(seq_total, LMAX, D)
    params = tuple((member.astype(jnp.float32) for member in (attn_gain, w_query, w_key, w_value, w_out, ffn_gain, w_gate, w_up, w_down)))
    single = jax.checkpoint(layer_one)

    def forward(params, patch_rows):
        dealt_rows = patch_rows[slot_owner]

        def scan_step(scan_carry, members):
            return (scan_carry, single(params, members[0], members[1]))
        return lax.scan(scan_step, jnp.zeros((), jnp.float32), (dealt_rows, own_lengths))[1]
    result, pullback = jax.vjp(forward, params, patch_rows)
    grad_params, grad_rows = pullback(cotangent.astype(jnp.float32).reshape(seq_total, LMAX, D))
    output = result.astype(jnp.bfloat16).reshape(cotangent.shape)
    grad_patches = grad_rows.astype(jnp.bfloat16).reshape(patches.shape)
    return (output, grad_patches, grad_params[0], grad_params[1], grad_params[2], grad_params[3], grad_params[4], grad_params[5], grad_params[6], grad_params[7], grad_params[8])
```

```python
import functools

import jax
import jax.numpy as jnp
from jax import lax
from jax.experimental import pallas as pl
from jax.experimental.pallas import tpu as pltpu
from jax.sharding import PartitionSpec as P

HEAD_DIM = 64
PAIR = 2 * HEAD_DIM
EPSILON = 1e-05
NEGATIVE = -1e30
LOW = jnp.bfloat16
F32 = jnp.float32


def dot(left, right, left_dim, right_dim, dtype=F32):
    return lax.dot_general(
        left, right, (((left_dim,), (right_dim,)), ((), ())), preferred_element_type=dtype
    )


def norm_rows(rows, gain_vector):
    factor = lax.rsqrt(jnp.mean(rows * rows, -1, keepdims=True) + EPSILON)
    return ((rows * factor * gain_vector).astype(LOW), factor)


def norm_back(rows, factor, gain_vector, upstream):
    scaled = upstream * gain_vector
    inward = factor * scaled - rows * factor**3 * jnp.mean(rows * scaled, -1, keepdims=True)
    return (inward, jnp.sum(upstream * rows * factor, 0))


def head_masks(rows):
    lane = lax.broadcasted_iota(jnp.int32, (rows, PAIR), 1)
    return (lane < HEAD_DIM, lane >= HEAD_DIM)


def attend_kernel(info, q_ref, k_ref, v_ref, o_ref, total_ref):
    block = q_ref.shape[0]
    number = pl.program_id(1)
    masks = head_masks(block)

    @pl.when(number < info[0])
    def _():
        query = q_ref[...] * jnp.asarray(HEAD_DIM**-0.5, LOW)
        queries = [jnp.where(m, query, jnp.zeros_like(query)) for m in masks]
        above = lax.broadcasted_iota(jnp.int32, (block, block), 0) >= lax.broadcasted_iota(
            jnp.int32, (block, block), 1
        )

        def step(key_number, state, diagonal):
            start = pl.multiple_of(info[1 + key_number] * block, block)
            keys = k_ref[pl.ds(start, block), :]
            values = v_ref[pl.ds(start, block), :]
            result = []
            for head in range(2):
                high, acc = state[head]
                scores = dot(queries[head], keys, 1, 1)
                if diagonal:
                    scores = jnp.where(above, scores, NEGATIVE)
                new_high = jnp.maximum(high, jnp.max(scores, -1, keepdims=True))
                probs = jnp.exp(scores - new_high).astype(LOW)
                extended = jnp.where(masks[head], values, jnp.ones_like(values))
                acc = acc * jnp.exp(high - new_high) + dot(probs, extended, 1, 0)
                result.append((new_high, acc))
            return tuple(result)

        start_state = tuple(
            (jnp.full((block, 1), NEGATIVE, F32), jnp.zeros((block, PAIR), F32)) for _ in range(2)
        )
        state = step(number, start_state, True)
        state = lax.fori_loop(0, number, lambda n, s: step(n, s, False), state)
        (high0, acc0), (high1, acc1) = state
        sum0 = acc0[:, HEAD_DIM : HEAD_DIM + 1]
        sum1 = acc1[:, 0:1]
        o_ref[...] = jnp.where(masks[0], acc0 / sum0, acc1 / sum1).astype(LOW)
        total_ref[...] = jnp.where(masks[0], high0 + jnp.log(sum0), high1 + jnp.log(sum1))

    @pl.when(number >= info[0])
    def _():
        o_ref[...] = jnp.zeros_like(o_ref)
        total_ref[...] = jnp.zeros_like(total_ref)


def attend(info, qkv, block):
    rows, width = qkv.shape
    pairs = width // (3 * PAIR)
    here = pl.BlockSpec((block, PAIR), lambda h, i, info: (info[1 + i], h))
    return pl.pallas_call(
        attend_kernel,
        grid_spec=pltpu.PrefetchScalarGridSpec(
            num_scalar_prefetch=1,
            grid=(pairs, rows // block),
            in_specs=[
                here,
                pl.BlockSpec((rows, PAIR), lambda h, i, info: (0, pairs + h)),
                pl.BlockSpec((rows, PAIR), lambda h, i, info: (0, 2 * pairs + h)),
            ],
            out_specs=[here, here],
        ),
        out_shape=[
            jax.ShapeDtypeStruct((rows, pairs * PAIR), LOW),
            jax.ShapeDtypeStruct((rows, pairs * PAIR), F32),
        ],
        name="attend",
    )(info, qkv, qkv, qkv)


def attend_back_kernel(
    block, info, q_ref, k_ref, v_ref, do_ref, o_ref, total_ref, dq_ref, dk_ref, dv_ref, dq_acc, dk_acc, dv_acc
):
    masks = head_masks(block)
    dk_acc[...] = jnp.zeros_like(dk_acc)
    dv_acc[...] = jnp.zeros_like(dv_acc)
    dq_ref[...] = jnp.zeros_like(dq_ref)
    below = lax.broadcasted_iota(jnp.int32, (block, block), 0) <= lax.broadcasted_iota(
        jnp.int32, (block, block), 1
    )

    def split(value):
        return [jnp.where(m, value, jnp.zeros_like(value)) for m in masks]

    def query_step(number, carry):
        start = pl.multiple_of(info[1 + number] * block, block)
        here = pl.ds(start, block)
        queries = split(q_ref[here, :] * jnp.asarray(HEAD_DIM**-0.5, LOW))
        grad = do_ref[here, :]
        grads = split(grad)
        product = (grad.astype(F32) * o_ref[here, :].astype(F32)).T
        row_dots = [
            jnp.sum(product[h * HEAD_DIM : (h + 1) * HEAD_DIM], 0, keepdims=True) for h in range(2)
        ]
        turned = total_ref[here, :].T
        totals = [turned[h * HEAD_DIM : h * HEAD_DIM + 1] for h in range(2)]
        dq_acc[...] = jnp.zeros_like(dq_acc)

        def key_step(key_number, diagonal):
            there = pl.ds(pl.multiple_of(info[1 + key_number] * block, block), block)
            keys = k_ref[there, :]
            values = v_ref[there, :]
            split_keys = split(keys)
            dq = dq_acc[...]
            dk = dk_acc[there, :]
            dv = dv_acc[there, :]
            for head in range(2):
                scores = dot(keys, queries[head], 1, 1)
                if diagonal:
                    scores = jnp.where(below, scores, NEGATIVE)
                probs = jnp.exp(scores - totals[head])
                grad_probs = dot(values, grads[head], 1, 1)
                grad_scores = (probs * (grad_probs - row_dots[head])).astype(LOW)
                dv = dv + dot(probs.astype(LOW), grads[head], 1, 0)
                dk = dk + dot(grad_scores, queries[head], 1, 0)
                dq = dq + dot(grad_scores, split_keys[head], 0, 0)
            dq_acc[...] = dq
            dk_acc[there, :] = dk
            dv_acc[there, :] = dv

        key_step(number, True)

        def loop_step(key_number, inner):
            key_step(key_number, False)
            return inner

        lax.fori_loop(0, number, loop_step, 0)
        dq_ref[here, :] = (dq_acc[...] * HEAD_DIM**-0.5).astype(LOW)
        return carry

    lax.fori_loop(0, info[0], query_step, 0)
    dk_ref[...] = dk_acc[...].astype(LOW)
    dv_ref[...] = dv_acc[...].astype(LOW)


def attend_back(info, qkv, grad_out, mixed, totals, block):
    rows, width = qkv.shape
    pairs = width // (3 * PAIR)

    def column(offset):
        return pl.BlockSpec((rows, PAIR), lambda h, info: (0, offset + h))

    shape = jax.ShapeDtypeStruct((rows, pairs * PAIR), LOW)
    return pl.pallas_call(
        functools.partial(attend_back_kernel, block),
        grid_spec=pltpu.PrefetchScalarGridSpec(
            num_scalar_prefetch=1,
            grid=(pairs,),
            in_specs=[column(0), column(pairs), column(2 * pairs), column(0), column(0), column(0)],
            out_specs=[column(0)] * 3,
            scratch_shapes=[
                pltpu.VMEM((block, PAIR), F32),
                pltpu.VMEM((rows, PAIR), F32),
                pltpu.VMEM((rows, PAIR), F32),
            ],
        ),
        out_shape=[shape] * 3,
        name="attend_back",
    )(info, qkv, qkv, qkv, grad_out, mixed, totals)


def after(value, *others):
    return lax.optimization_barrier((value,) + others)[0]


def local(
    patches,
    lengths,
    deal,
    attn_gain,
    w_query,
    w_key,
    w_value,
    w_out,
    ffn_gain,
    w_gate,
    w_up,
    w_down,
    cotangent,
):
    groups = lax.axis_size("dp")
    seq_total = patches.shape[0]
    band = patches.shape[2]
    quarter = cotangent.shape[2]
    width = patches.shape[3]
    group = lax.axis_index("dp")
    place = lax.axis_index("tensor")
    chip = place // 2
    core = place % 2

    def swap_core(value):
        return lax.ppermute(value, "tensor", [(0, 1), (1, 0), (2, 3), (3, 2)])

    def swap_chip(value):
        return lax.ppermute(value, "tensor", [(0, 2), (2, 0), (1, 3), (3, 1)])

    slot_owner = jnp.argsort(deal)
    owners = slot_owner.reshape(groups, 2)
    mine = jnp.take(owners, chip, axis=1)
    theirs = jnp.take(owners, 1 - chip, axis=1)
    length = lengths[mine[group]]
    given = swap_chip(patches[theirs, 0])
    sent = jnp.stack((patches[mine, 0], given), 1)
    arrived = lax.all_to_all(sent, "dp", split_axis=0, concat_axis=0, tiled=True)
    inputs = arrived.transpose(1, 0, 2, 3).reshape(2 * quarter, width).astype(F32)

    w_qkv = jnp.concatenate((w_query, w_key, w_value), 1)
    w_qkv_far, w_out_far = swap_chip((after(w_qkv, given), after(w_out, given)))
    w_gate_far, w_up_far, w_down_far = swap_chip(
        tuple(after(w, w_qkv_far) for w in (w_gate, w_up, w_down))
    )
    cot_near = jnp.take(cotangent[:, 0], chip, axis=0)
    cot_far = swap_chip(after(jnp.take(cotangent[:, 0], 1 - chip, axis=0), w_qkv_far))

    numbers = jnp.arange(4)
    slots = 2 * (numbers % 2 != core) + (numbers // 2 != chip)
    live_blocks = (length + quarter - 1) // quarter
    info = jnp.concatenate((live_blocks[None], slots)).astype(jnp.int32)
    offsets = jnp.arange(quarter)
    positions = jnp.concatenate(
        ((2 * chip + core) * quarter + offsets, (2 * (1 - chip) + core) * quarter + offsets)
    )
    live_rows = (positions < length).astype(F32)[:, None]
    own_rows = 2 * quarter

    def gather(value):
        return jnp.concatenate((value, swap_core(value)), 0)

    def scatter(make):
        far = swap_core(make(slice(own_rows, None)).astype(LOW))
        return make(slice(0, own_rows)) + far.astype(F32)

    normed_attn, factor_attn = norm_rows(inputs, attn_gain)
    rows_attn = gather(normed_attn)
    qkv = [dot(rows_attn, w, 1, 0, LOW) for w in (w_qkv, w_qkv_far)]
    mixed_near, total_near = attend(info, qkv[0], quarter)
    mixed_far, total_far = attend(info, qkv[1], quarter)
    attention = scatter(
        lambda part: dot(mixed_near[part], w_out, 1, 0) + dot(mixed_far[part], w_out_far, 1, 0)
    )
    hidden = inputs + attention
    normed_ffn, factor_ffn = norm_rows(hidden, ffn_gain)
    rows_ffn = gather(normed_ffn)
    gates = jnp.concatenate((w_gate, w_gate_far), 1)
    ups = jnp.concatenate((w_up, w_up_far), 1)
    downs = jnp.concatenate((w_down, w_down_far), 0)
    gate_pre = dot(rows_ffn, gates, 1, 0)
    up_proj = dot(rows_ffn, ups, 1, 0)
    sigmoid = 1.0 / (1.0 + jnp.exp(-gate_pre))
    swish_gate = gate_pre * sigmoid
    product = (swish_gate * up_proj).astype(LOW)
    feedforward = scatter(lambda part: dot(product[part], downs, 1, 0))
    result = (live_rows * (hidden + feedforward)).astype(LOW)
    result_far = swap_chip(result[quarter:])
    output = jnp.where(
        chip == 0,
        jnp.stack((result[:quarter], result_far)),
        jnp.stack((result_far, result[:quarter])),
    )[:, None]

    grad_result = jnp.concatenate((cot_near, cot_far), 0).astype(F32) * live_rows
    grad_ffn = gather(grad_result.astype(LOW))
    grad_product = dot(grad_ffn, downs, 1, 1)
    grad_gate = (grad_product * up_proj * sigmoid * (1.0 + gate_pre * (1.0 - sigmoid))).astype(LOW)
    grad_up = (grad_product * swish_gate).astype(LOW)

    half = w_gate.shape[1]

    def over_chips(parts, ahead=()):
        far = swap_chip(jnp.concatenate([far.astype(LOW) for _, far in parts], 0))
        summed = jnp.concatenate([near for near, _ in parts], 0) + far.astype(F32)
        spread = summed.astype(LOW).reshape(-1, groups, width // groups).transpose(1, 0, 2)
        moved = lax.all_to_all(spread, "dp", split_axis=0, concat_axis=0, tiled=True)
        return jnp.sum(moved.astype(F32), 0)

    def halves(value):
        return (value[:half], value[half:])

    ffn_shards = over_chips(
        [
            halves(dot(product, grad_ffn, 0, 0)),
            halves(dot(grad_gate, rows_ffn, 0, 0)),
            halves(dot(grad_up, rows_ffn, 0, 0)),
        ]
    )
    grad_normed_ffn = scatter(
        lambda part: dot(grad_gate[part], gates, 1, 1) + dot(grad_up[part], ups, 1, 1)
    )
    grad_hidden, gain_ffn_part = norm_back(hidden, factor_ffn, ffn_gain, grad_normed_ffn)
    grad_hidden = grad_hidden + grad_result
    grad_attn = gather(grad_hidden.astype(LOW))
    out_shard = over_chips([(dot(mixed_near, grad_attn, 0, 0), dot(mixed_far, grad_attn, 0, 0))])
    grad_far = attend_back(
        info, qkv[1], dot(grad_attn, w_out_far, 1, 1, LOW), mixed_far, total_far, quarter
    )
    grad_near = attend_back(
        info, qkv[0], dot(grad_attn, w_out, 1, 1, LOW), mixed_near, total_near, quarter
    )
    grad_far = jnp.concatenate(grad_far, 1)
    grad_near = jnp.concatenate(grad_near, 1)
    grad_normed_attn = scatter(
        lambda part: dot(grad_near[part], w_qkv, 1, 1) + dot(grad_far[part], w_qkv_far, 1, 1)
    )
    qkv_shards = over_chips([(dot(grad_near, rows_attn, 0, 0), dot(grad_far, rows_attn, 0, 0))])
    grad_inputs, gain_attn_part = norm_back(inputs, factor_attn, attn_gain, grad_normed_attn)
    grad_inputs = (grad_inputs + grad_hidden).astype(LOW)
    returned = lax.all_to_all(
        grad_inputs.reshape(2, groups, band, width).transpose(1, 0, 2, 3),
        "dp",
        split_axis=0,
        concat_axis=0,
        tiled=True,
    )
    back_near = returned[:, 0]
    back_far = swap_chip(returned[:, 1])
    by_slot = jnp.where(
        chip == 0, jnp.stack((back_near, back_far), 1), jnp.stack((back_far, back_near), 1)
    ).reshape(seq_total, band, width)
    grad_patches = by_slot[deal][:, None]

    def total_of(value):
        value = value + swap_core(value)
        value = value + swap_chip(value)
        step = 1
        while step < groups:
            value = value + lax.ppermute(value, "dp", [(i, i ^ step) for i in range(groups)])
            step *= 2
        return value

    gain_grads = total_of(jnp.stack((gain_attn_part, gain_ffn_part)))
    part = w_query.shape[1]
    return (
        output,
        grad_patches,
        gain_grads[0],
        qkv_shards[:part].T,
        qkv_shards[part : 2 * part].T,
        qkv_shards[2 * part :].T,
        out_shard,
        gain_grads[1],
        ffn_shards[half : 2 * half].T,
        ffn_shards[2 * half :].T,
        ffn_shards[:half],
    )


def solution(mesh):
    in_specs = (
        P(None, "tensor", "dp", None),
        P(),
        P(),
        P(),
        P(None, "tensor"),
        P(None, "tensor"),
        P(None, "tensor"),
        P("tensor", None),
        P(),
        P(None, "tensor"),
        P(None, "tensor"),
        P("tensor", None),
        P("dp", "tensor", None, None),
    )
    out_specs = (
        P("dp", "tensor", None, None),
        P(None, "tensor", "dp", None),
        P(),
        P("dp", "tensor"),
        P("dp", "tensor"),
        P("dp", "tensor"),
        P("tensor", "dp"),
        P(),
        P("dp", "tensor"),
        P("dp", "tensor"),
        P("tensor", "dp"),
    )
    return jax.shard_map(local, mesh=mesh, in_specs=in_specs, out_specs=out_specs, check_vma=False)
```

```python
import functools

import jax
import jax.numpy as jnp
from jax import lax
from jax.experimental import pallas as pl
from jax.experimental.pallas import tpu as pltpu
from jax.sharding import PartitionSpec as P


HEAD_DIM = 64
PAIR = 2 * HEAD_DIM
EPSILON = 1e-05
NEGATIVE = -1e30
LOW = jnp.bfloat16
F32 = jnp.float32


def dot(left, right, left_dim, right_dim, dtype=F32):
    return lax.dot_general(
        left, right, (((left_dim,), (right_dim,)), ((), ())), preferred_element_type=dtype
    )


def norm_rows(rows, gain_vector):
    factor = lax.rsqrt(jnp.mean(rows * rows, -1, keepdims=True) + EPSILON)
    return ((rows * factor * gain_vector).astype(LOW), factor)


def norm_back(rows, factor, gain_vector, upstream):
    scaled = upstream * gain_vector
    inward = factor * scaled - rows * factor**3 * jnp.mean(rows * scaled, -1, keepdims=True)
    return (inward, jnp.sum(upstream * rows * factor, 0))


def head_masks(rows):
    lane = lax.broadcasted_iota(jnp.int32, (rows, PAIR), 1)
    return (lane < HEAD_DIM, lane >= HEAD_DIM)


def attend_kernel(info, q_ref, k_ref, v_ref, o_ref, total_ref):
    block = q_ref.shape[0]
    number = pl.program_id(1)
    masks = head_masks(block)

    @pl.when(number < info[0])
    def _():
        query = q_ref[...] * jnp.asarray(HEAD_DIM**-0.5, LOW)
        queries = [jnp.where(m, query, jnp.zeros_like(query)) for m in masks]
        above = lax.broadcasted_iota(jnp.int32, (block, block), 0) >= lax.broadcasted_iota(
            jnp.int32, (block, block), 1
        )

        def step(key_number, state, diagonal):
            start = pl.multiple_of(info[1 + key_number] * block, block)
            keys = k_ref[pl.ds(start, block), :]
            values = v_ref[pl.ds(start, block), :]
            result = []
            for head in range(2):
                high, acc = state[head]
                scores = dot(queries[head], keys, 1, 1)
                if diagonal:
                    scores = jnp.where(above, scores, NEGATIVE)
                new_high = jnp.maximum(high, jnp.max(scores, -1, keepdims=True))
                probs = jnp.exp(scores - new_high).astype(LOW)
                extended = jnp.where(masks[head], values, jnp.ones_like(values))
                acc = acc * jnp.exp(high - new_high) + dot(probs, extended, 1, 0)
                result.append((new_high, acc))
            return tuple(result)

        start_state = tuple(
            (jnp.full((block, 1), NEGATIVE, F32), jnp.zeros((block, PAIR), F32)) for _ in range(2)
        )
        state = step(number, start_state, True)
        state = lax.fori_loop(0, number, lambda n, s: step(n, s, False), state)
        (high0, acc0), (high1, acc1) = state
        sum0 = acc0[:, HEAD_DIM : HEAD_DIM + 1]
        sum1 = acc1[:, 0:1]
        o_ref[...] = jnp.where(masks[0], acc0 / sum0, acc1 / sum1).astype(LOW)
        total_ref[...] = jnp.where(masks[0], high0 + jnp.log(sum0), high1 + jnp.log(sum1))

    @pl.when(number >= info[0])
    def _():
        o_ref[...] = jnp.zeros_like(o_ref)
        total_ref[...] = jnp.zeros_like(total_ref)


def attend(info, qkv, block):
    rows, width = qkv.shape
    pairs = width // (3 * PAIR)
    here = pl.BlockSpec((block, PAIR), lambda h, i, info: (info[1 + i], h))
    return pl.pallas_call(
        attend_kernel,
        grid_spec=pltpu.PrefetchScalarGridSpec(
            num_scalar_prefetch=1,
            grid=(pairs, rows // block),
            in_specs=[
                here,
                pl.BlockSpec((rows, PAIR), lambda h, i, info: (0, pairs + h)),
                pl.BlockSpec((rows, PAIR), lambda h, i, info: (0, 2 * pairs + h)),
            ],
            out_specs=[here, here],
        ),
        out_shape=[
            jax.ShapeDtypeStruct((rows, pairs * PAIR), LOW),
            jax.ShapeDtypeStruct((rows, pairs * PAIR), F32),
        ],
        name="attend",
    )(info, qkv, qkv, qkv)


def attend_back_kernel(
    block, info, q_ref, k_ref, v_ref, do_ref, o_ref, total_ref, dq_ref, dk_ref, dv_ref, dq_acc, dk_acc, dv_acc
):
    masks = head_masks(block)
    dk_acc[...] = jnp.zeros_like(dk_acc)
    dv_acc[...] = jnp.zeros_like(dv_acc)
    dq_ref[...] = jnp.zeros_like(dq_ref)
    below = lax.broadcasted_iota(jnp.int32, (block, block), 0) <= lax.broadcasted_iota(
        jnp.int32, (block, block), 1
    )

    def split(value):
        return [jnp.where(m, value, jnp.zeros_like(value)) for m in masks]

    def query_step(number, carry):
        start = pl.multiple_of(info[1 + number] * block, block)
        here = pl.ds(start, block)
        queries = split(q_ref[here, :] * jnp.asarray(HEAD_DIM**-0.5, LOW))
        grad = do_ref[here, :]
        grads = split(grad)
        product = (grad.astype(F32) * o_ref[here, :].astype(F32)).T
        row_dots = [
            jnp.sum(product[h * HEAD_DIM : (h + 1) * HEAD_DIM], 0, keepdims=True) for h in range(2)
        ]
        turned = total_ref[here, :].T
        totals = [turned[h * HEAD_DIM : h * HEAD_DIM + 1] for h in range(2)]
        dq_acc[...] = jnp.zeros_like(dq_acc)

        def key_step(key_number, diagonal):
            there = pl.ds(pl.multiple_of(info[1 + key_number] * block, block), block)
            keys = k_ref[there, :]
            values = v_ref[there, :]
            split_keys = split(keys)
            dq = dq_acc[...]
            dk = dk_acc[there, :]
            dv = dv_acc[there, :]
            for head in range(2):
                scores = dot(keys, queries[head], 1, 1)
                if diagonal:
                    scores = jnp.where(below, scores, NEGATIVE)
                probs = jnp.exp(scores - totals[head])
                grad_probs = dot(values, grads[head], 1, 1)
                grad_scores = (probs * (grad_probs - row_dots[head])).astype(LOW)
                dv = dv + dot(probs.astype(LOW), grads[head], 1, 0)
                dk = dk + dot(grad_scores, queries[head], 1, 0)
                dq = dq + dot(grad_scores, split_keys[head], 0, 0)
            dq_acc[...] = dq
            dk_acc[there, :] = dk
            dv_acc[there, :] = dv

        key_step(number, True)

        def loop_step(key_number, inner):
            key_step(key_number, False)
            return inner

        lax.fori_loop(0, number, loop_step, 0)
        dq_ref[here, :] = (dq_acc[...] * HEAD_DIM**-0.5).astype(LOW)
        return carry

    lax.fori_loop(0, info[0], query_step, 0)
    dk_ref[...] = dk_acc[...].astype(LOW)
    dv_ref[...] = dv_acc[...].astype(LOW)


def attend_back(info, qkv, grad_out, mixed, totals, block):
    rows, width = qkv.shape
    pairs = width // (3 * PAIR)

    def column(offset):
        return pl.BlockSpec((rows, PAIR), lambda h, info: (0, offset + h))

    shape = jax.ShapeDtypeStruct((rows, pairs * PAIR), LOW)
    return pl.pallas_call(
        functools.partial(attend_back_kernel, block),
        grid_spec=pltpu.PrefetchScalarGridSpec(
            num_scalar_prefetch=1,
            grid=(pairs,),
            in_specs=[column(0), column(pairs), column(2 * pairs), column(0), column(0), column(0)],
            out_specs=[column(0)] * 3,
            scratch_shapes=[
                pltpu.VMEM((block, PAIR), F32),
                pltpu.VMEM((rows, PAIR), F32),
                pltpu.VMEM((rows, PAIR), F32),
            ],
        ),
        out_shape=[shape] * 3,
        name="attend_back",
    )(info, qkv, qkv, qkv, grad_out, mixed, totals)


def after(value, *others):
    return lax.optimization_barrier((value,) + others)[0]


def layer(
    patches,
    lengths,
    deal,
    attn_gain,
    w_query,
    w_key,
    w_value,
    w_out,
    ffn_gain,
    w_gate,
    w_up,
    w_down,
    cotangent,
):
    groups = lax.axis_size("dp")
    seq_total = patches.shape[0]
    band = patches.shape[2]
    quarter = cotangent.shape[2]
    width = patches.shape[3]
    group = lax.axis_index("dp")
    place = lax.axis_index("tensor")
    chip = place // 2
    core = place % 2

    def swap_core(value):
        return lax.ppermute(value, "tensor", [(0, 1), (1, 0), (2, 3), (3, 2)])

    def swap_chip(value):
        return lax.ppermute(value, "tensor", [(0, 2), (2, 0), (1, 3), (3, 1)])

    def exchange(value):
        return lax.all_to_all(value, "dp", split_axis=0, concat_axis=0, tiled=True)

    slot_owner = jnp.argsort(deal)
    owners = slot_owner.reshape(groups, 2)
    mine = jnp.take(owners, chip, axis=1)
    theirs = jnp.take(owners, 1 - chip, axis=1)
    length = lengths[mine[group]]
    given = swap_chip(patches[theirs, 0])
    arrived_near = exchange(patches[mine, 0])
    arrived_far = exchange(given)
    inputs = jnp.stack((arrived_near, arrived_far)).reshape(2 * quarter, width).astype(F32)

    w_qkv = jnp.concatenate((w_query, w_key, w_value), 1)
    w_qkv_far = swap_chip(after(w_qkv, given))
    w_out_far = swap_chip(after(w_out, given))
    w_gate_far = swap_chip(after(w_gate, arrived_far))
    w_up_far = swap_chip(after(w_up, arrived_far))
    w_down_far = swap_chip(after(w_down, arrived_far))
    cot_near = jnp.take(cotangent[:, 0], chip, axis=0)
    cot_far = swap_chip(after(jnp.take(cotangent[:, 0], 1 - chip, axis=0), arrived_far))

    numbers = jnp.arange(4)
    slots = 2 * (numbers % 2 != core) + (numbers // 2 != chip)
    live_blocks = (length + quarter - 1) // quarter
    info = jnp.concatenate((live_blocks[None], slots)).astype(jnp.int32)
    offsets = jnp.arange(quarter)
    positions = jnp.concatenate(
        ((2 * chip + core) * quarter + offsets, (2 * (1 - chip) + core) * quarter + offsets)
    )
    live_rows = (positions < length).astype(F32)[:, None]
    own_rows = 2 * quarter

    def gather(value):
        return jnp.concatenate((value, swap_core(value)), 0)

    def scatter(make):
        far = swap_core(make(slice(own_rows, None)).astype(LOW))
        return make(slice(0, own_rows)) + far.astype(F32)

    normed_attn, factor_attn = norm_rows(inputs, attn_gain)
    rows_attn = gather(normed_attn)
    qkv = [dot(rows_attn, w, 1, 0, LOW) for w in (w_qkv, w_qkv_far)]
    mixed_near, total_near = attend(info, qkv[0], quarter)
    mixed_far, total_far = attend(info, qkv[1], quarter)
    attention = scatter(
        lambda part: dot(mixed_near[part], w_out, 1, 0) + dot(mixed_far[part], w_out_far, 1, 0)
    )
    hidden = inputs + attention
    normed_ffn, factor_ffn = norm_rows(hidden, ffn_gain)
    rows_ffn = gather(normed_ffn)
    gates = jnp.concatenate((w_gate, w_gate_far), 1)
    ups = jnp.concatenate((w_up, w_up_far), 1)
    downs = jnp.concatenate((w_down, w_down_far), 0)
    gate_pre = dot(rows_ffn, gates, 1, 0)
    up_proj = dot(rows_ffn, ups, 1, 0)
    sigmoid = 1.0 / (1.0 + jnp.exp(-gate_pre))
    swish_gate = gate_pre * sigmoid
    product = (swish_gate * up_proj).astype(LOW)
    feedforward = scatter(lambda part: dot(product[part], downs, 1, 0))
    result = (live_rows * (hidden + feedforward)).astype(LOW)
    result_far = swap_chip(result[quarter:])
    output = jnp.where(
        chip == 0,
        jnp.stack((result[:quarter], result_far)),
        jnp.stack((result_far, result[:quarter])),
    )[:, None]

    grad_result = jnp.concatenate((cot_near, cot_far), 0).astype(F32) * live_rows
    grad_ffn = gather(grad_result.astype(LOW))
    grad_product = dot(grad_ffn, downs, 1, 1)
    grad_gate = (grad_product * up_proj * sigmoid * (1.0 + gate_pre * (1.0 - sigmoid))).astype(LOW)
    grad_up = (grad_product * swish_gate).astype(LOW)

    half = w_gate.shape[1]

    def over_chips(parts):
        far = swap_chip(jnp.concatenate([far.astype(LOW) for _, far in parts], 0))
        summed = jnp.concatenate([near for near, _ in parts], 0) + far.astype(F32)
        spread = summed.astype(LOW).reshape(-1, groups, width // groups).transpose(1, 0, 2)
        return jnp.sum(exchange(spread).astype(F32), 0)

    def halves(value):
        return (value[:half], value[half:])

    down_shard = over_chips([halves(dot(product, grad_ffn, 0, 0))])
    up_halves = halves(dot(grad_up, rows_ffn, 0, 0))
    gate_up_shards = over_chips([halves(dot(grad_gate, rows_ffn, 0, 0)), up_halves])
    grad_normed_ffn = scatter(
        lambda part: dot(grad_gate[part], gates, 1, 1) + dot(grad_up[part], ups, 1, 1)
    )
    grad_hidden, gain_ffn_part = norm_back(hidden, factor_ffn, ffn_gain, grad_normed_ffn)
    grad_hidden = grad_hidden + grad_result
    grad_attn = gather(grad_hidden.astype(LOW))
    out_halves = (dot(mixed_near, grad_attn, 0, 0), dot(mixed_far, grad_attn, 0, 0))
    back_far = dot(grad_attn, w_out_far, 1, 1, LOW)
    grad_far = attend_back(info, qkv[1], back_far, mixed_far, total_far, quarter)
    grad_far = jnp.concatenate(grad_far, 1)
    weight_far = dot(grad_far, rows_attn, 0, 0, LOW)
    back_near = after(dot(grad_attn, w_out, 1, 1, LOW), weight_far)
    grad_near = attend_back(info, qkv[0], back_near, mixed_near, total_near, quarter)
    grad_near = jnp.concatenate(grad_near, 1)
    grad_normed_attn = scatter(
        lambda part: dot(grad_near[part], w_qkv, 1, 1) + dot(grad_far[part], w_qkv_far, 1, 1)
    )
    qkv_shards = over_chips([out_halves, (dot(grad_near, rows_attn, 0, 0), weight_far)])
    grad_inputs, gain_attn_part = norm_back(inputs, factor_attn, attn_gain, grad_normed_attn)
    grad_inputs = (grad_inputs + grad_hidden).astype(LOW)
    returned = exchange(grad_inputs[quarter:].reshape(groups, band, width))
    by_far = swap_chip(returned)
    by_near = exchange(grad_inputs[:quarter].reshape(groups, band, width))
    by_slot = jnp.where(
        chip == 0, jnp.stack((by_near, by_far), 1), jnp.stack((by_far, by_near), 1)
    ).reshape(seq_total, band, width)
    grad_patches = by_slot[deal][:, None]

    def total_of(value):
        value = value + swap_core(value)
        value = value + swap_chip(value)
        step = 1
        while step < groups:
            value = value + lax.ppermute(value, "dp", [(i, i ^ step) for i in range(groups)])
            step *= 2
        return value

    gain_grads = total_of(jnp.stack((gain_attn_part, gain_ffn_part)))
    part = w_query.shape[1]
    return (
        output,
        grad_patches,
        gain_grads[0],
        qkv_shards[part : 2 * part].T,
        qkv_shards[2 * part : 3 * part].T,
        qkv_shards[3 * part :].T,
        qkv_shards[:part],
        gain_grads[1],
        gate_up_shards[:half].T,
        gate_up_shards[half:].T,
        down_shard,
    )


def solution(mesh):
    in_specs = (
        P(None, "tensor", "dp", None),
        P(),
        P(),
        P(),
        P(None, "tensor"),
        P(None, "tensor"),
        P(None, "tensor"),
        P("tensor", None),
        P(),
        P(None, "tensor"),
        P(None, "tensor"),
        P("tensor", None),
        P("dp", "tensor", None, None),
    )
    out_specs = (
        P("dp", "tensor", None, None),
        P(None, "tensor", "dp", None),
        P(),
        P("dp", "tensor"),
        P("dp", "tensor"),
        P("dp", "tensor"),
        P("tensor", "dp"),
        P(),
        P("dp", "tensor"),
        P("dp", "tensor"),
        P("tensor", "dp"),
    )
    return jax.shard_map(layer, mesh=mesh, in_specs=in_specs, out_specs=out_specs, check_vma=False)
```

```python
import functools

import jax
import jax.numpy as jnp
from jax import lax
from jax.experimental import pallas as pl
from jax.experimental.pallas import tpu as pltpu
from jax.sharding import PartitionSpec as P


HEAD_DIM = 64
PAIR = 2 * HEAD_DIM
EPSILON = 1e-05
NEGATIVE = -1e30
LOW = jnp.bfloat16
F32 = jnp.float32


def dot(left, right, left_dim, right_dim, dtype=F32):
    return lax.dot_general(
        left, right, (((left_dim,), (right_dim,)), ((), ())), preferred_element_type=dtype
    )


def norm_rows(rows, gain_vector):
    factor = lax.rsqrt(jnp.mean(rows * rows, -1, keepdims=True) + EPSILON)
    return ((rows * factor * gain_vector).astype(LOW), factor)


def norm_back(rows, factor, gain_vector, upstream):
    scaled = upstream * gain_vector
    inward = factor * scaled - rows * factor**3 * jnp.mean(rows * scaled, -1, keepdims=True)
    return (inward, jnp.sum(upstream * rows * factor, 0))


def head_masks(rows):
    lane = lax.broadcasted_iota(jnp.int32, (rows, PAIR), 1)
    return (lane < HEAD_DIM, lane >= HEAD_DIM)


def attend_kernel(info, q_ref, k_ref, v_ref, o_ref, total_ref):
    block = q_ref.shape[0]
    number = pl.program_id(1)
    masks = head_masks(block)

    @pl.when(number < info[0])
    def _():
        query = q_ref[...] * jnp.asarray(HEAD_DIM**-0.5, LOW)
        queries = [jnp.where(m, query, jnp.zeros_like(query)) for m in masks]
        above = lax.broadcasted_iota(jnp.int32, (block, block), 0) >= lax.broadcasted_iota(
            jnp.int32, (block, block), 1
        )

        def step(key_number, state, diagonal):
            start = pl.multiple_of(info[1 + key_number] * block, block)
            keys = k_ref[pl.ds(start, block), :]
            values = v_ref[pl.ds(start, block), :]
            result = []
            for head in range(2):
                high, acc = state[head]
                scores = dot(queries[head], keys, 1, 1)
                if diagonal:
                    scores = jnp.where(above, scores, NEGATIVE)
                new_high = jnp.maximum(high, jnp.max(scores, -1, keepdims=True))
                probs = jnp.exp(scores - new_high).astype(LOW)
                extended = jnp.where(masks[head], values, jnp.ones_like(values))
                acc = acc * jnp.exp(high - new_high) + dot(probs, extended, 1, 0)
                result.append((new_high, acc))
            return tuple(result)

        start_state = tuple(
            (jnp.full((block, 1), NEGATIVE, F32), jnp.zeros((block, PAIR), F32)) for _ in range(2)
        )
        state = step(number, start_state, True)
        state = lax.fori_loop(0, number, lambda n, s: step(n, s, False), state)
        (high0, acc0), (high1, acc1) = state
        sum0 = acc0[:, HEAD_DIM : HEAD_DIM + 1]
        sum1 = acc1[:, 0:1]
        o_ref[...] = jnp.where(masks[0], acc0 / sum0, acc1 / sum1).astype(LOW)
        total_ref[...] = jnp.where(masks[0], high0 + jnp.log(sum0), high1 + jnp.log(sum1))

    @pl.when(number >= info[0])
    def _():
        o_ref[...] = jnp.zeros_like(o_ref)
        total_ref[...] = jnp.zeros_like(total_ref)


def attend(info, qkv, block):
    rows, width = qkv.shape
    pairs = width // (3 * PAIR)
    here = pl.BlockSpec((block, PAIR), lambda h, i, info: (info[1 + i], h))
    return pl.pallas_call(
        attend_kernel,
        grid_spec=pltpu.PrefetchScalarGridSpec(
            num_scalar_prefetch=1,
            grid=(pairs, rows // block),
            in_specs=[
                here,
                pl.BlockSpec((rows, PAIR), lambda h, i, info: (0, pairs + h)),
                pl.BlockSpec((rows, PAIR), lambda h, i, info: (0, 2 * pairs + h)),
            ],
            out_specs=[here, here],
        ),
        out_shape=[
            jax.ShapeDtypeStruct((rows, pairs * PAIR), LOW),
            jax.ShapeDtypeStruct((rows, pairs * PAIR), F32),
        ],
        name="attend",
    )(info, qkv, qkv, qkv)


def attend_back_kernel(
    block, info, q_ref, k_ref, v_ref, do_ref, o_ref, total_ref, dq_ref, dk_ref, dv_ref, dq_acc, dk_acc, dv_acc
):
    masks = head_masks(block)
    dk_acc[...] = jnp.zeros_like(dk_acc)
    dv_acc[...] = jnp.zeros_like(dv_acc)
    dq_ref[...] = jnp.zeros_like(dq_ref)
    below = lax.broadcasted_iota(jnp.int32, (block, block), 0) <= lax.broadcasted_iota(
        jnp.int32, (block, block), 1
    )

    def split(value):
        return [jnp.where(m, value, jnp.zeros_like(value)) for m in masks]

    def query_step(number, carry):
        start = pl.multiple_of(info[1 + number] * block, block)
        here = pl.ds(start, block)
        queries = split(q_ref[here, :] * jnp.asarray(HEAD_DIM**-0.5, LOW))
        grad = do_ref[here, :]
        grads = split(grad)
        product = (grad.astype(F32) * o_ref[here, :].astype(F32)).T
        row_dots = [
            jnp.sum(product[h * HEAD_DIM : (h + 1) * HEAD_DIM], 0, keepdims=True) for h in range(2)
        ]
        turned = total_ref[here, :].T
        totals = [turned[h * HEAD_DIM : h * HEAD_DIM + 1] for h in range(2)]
        dq_acc[...] = jnp.zeros_like(dq_acc)

        def key_step(key_number, diagonal):
            there = pl.ds(pl.multiple_of(info[1 + key_number] * block, block), block)
            keys = k_ref[there, :]
            values = v_ref[there, :]
            split_keys = split(keys)
            dq = dq_acc[...]
            dk = dk_acc[there, :]
            dv = dv_acc[there, :]
            for head in range(2):
                scores = dot(keys, queries[head], 1, 1)
                if diagonal:
                    scores = jnp.where(below, scores, NEGATIVE)
                probs = jnp.exp(scores - totals[head])
                grad_probs = dot(values, grads[head], 1, 1)
                grad_scores = (probs * (grad_probs - row_dots[head])).astype(LOW)
                dv = dv + dot(probs.astype(LOW), grads[head], 1, 0)
                dk = dk + dot(grad_scores, queries[head], 1, 0)
                dq = dq + dot(grad_scores, split_keys[head], 0, 0)
            dq_acc[...] = dq
            dk_acc[there, :] = dk
            dv_acc[there, :] = dv

        key_step(number, True)

        def loop_step(key_number, inner):
            key_step(key_number, False)
            return inner

        lax.fori_loop(0, number, loop_step, 0)
        dq_ref[here, :] = (dq_acc[...] * HEAD_DIM**-0.5).astype(LOW)
        return carry

    lax.fori_loop(0, info[0], query_step, 0)
    dk_ref[...] = dk_acc[...].astype(LOW)
    dv_ref[...] = dv_acc[...].astype(LOW)


def attend_back(info, qkv, grad_out, mixed, totals, block):
    rows, width = qkv.shape
    pairs = width // (3 * PAIR)

    def column(offset):
        return pl.BlockSpec((rows, PAIR), lambda h, info: (0, offset + h))

    shape = jax.ShapeDtypeStruct((rows, pairs * PAIR), LOW)
    return pl.pallas_call(
        functools.partial(attend_back_kernel, block),
        grid_spec=pltpu.PrefetchScalarGridSpec(
            num_scalar_prefetch=1,
            grid=(pairs,),
            in_specs=[column(0), column(pairs), column(2 * pairs), column(0), column(0), column(0)],
            out_specs=[column(0)] * 3,
            scratch_shapes=[
                pltpu.VMEM((block, PAIR), F32),
                pltpu.VMEM((rows, PAIR), F32),
                pltpu.VMEM((rows, PAIR), F32),
            ],
        ),
        out_shape=[shape] * 3,
        name="attend_back",
    )(info, qkv, qkv, qkv, grad_out, mixed, totals)


def after(value, *others):
    return lax.optimization_barrier((value,) + others)[0]


def layer(
    patches,
    lengths,
    deal,
    attn_gain,
    w_query,
    w_key,
    w_value,
    w_out,
    ffn_gain,
    w_gate,
    w_up,
    w_down,
    cotangent,
):
    groups = lax.axis_size("dp")
    seq_total = patches.shape[0]
    band = patches.shape[2]
    quarter = cotangent.shape[2]
    width = patches.shape[3]
    group = lax.axis_index("dp")
    place = lax.axis_index("tensor")
    chip = place // 2
    core = place % 2

    def swap_core(value):
        return lax.ppermute(value, "tensor", [(0, 1), (1, 0), (2, 3), (3, 2)])

    def swap_chip(value):
        return lax.ppermute(value, "tensor", [(0, 2), (2, 0), (1, 3), (3, 1)])

    def exchange(value):
        return lax.all_to_all(value, "dp", split_axis=0, concat_axis=0, tiled=True)

    slot_owner = jnp.argsort(deal)
    owners = slot_owner.reshape(groups, 2)
    mine = jnp.take(owners, chip, axis=1)
    theirs = jnp.take(owners, 1 - chip, axis=1)
    length = lengths[mine[group]]
    given = swap_chip(patches[theirs, 0])
    arrived_near = exchange(patches[mine, 0])
    arrived_far = exchange(given)
    inputs = jnp.stack((arrived_near, arrived_far)).reshape(2 * quarter, width).astype(F32)

    w_qkv = jnp.concatenate((w_query, w_key, w_value), 1)
    w_qkv_far = swap_chip(after(w_qkv, given))
    w_out_far = swap_chip(after(w_out, given))
    w_gate_far = swap_chip(after(w_gate, arrived_far))
    w_up_far = swap_chip(after(w_up, arrived_far))
    w_down_far = swap_chip(after(w_down, arrived_far))
    cot_near = jnp.take(cotangent[:, 0], chip, axis=0)
    cot_far = swap_chip(after(jnp.take(cotangent[:, 0], 1 - chip, axis=0), arrived_far))

    numbers = jnp.arange(4)
    slots = 2 * (numbers % 2 != core) + (numbers // 2 != chip)
    live_blocks = (length + quarter - 1) // quarter
    info = jnp.concatenate((live_blocks[None], slots)).astype(jnp.int32)
    offsets = jnp.arange(quarter)
    positions = jnp.concatenate(
        ((2 * chip + core) * quarter + offsets, (2 * (1 - chip) + core) * quarter + offsets)
    )
    live_rows = (positions < length).astype(F32)[:, None]
    own_rows = 2 * quarter

    def gather(value):
        return jnp.concatenate((value, swap_core(value)), 0)

    def scatter(make):
        far = swap_core(make(slice(own_rows, None)).astype(LOW))
        return make(slice(0, own_rows)) + far.astype(F32)

    normed_attn, factor_attn = norm_rows(inputs, attn_gain)
    rows_attn = gather(normed_attn)
    qkv = [dot(rows_attn, w, 1, 0, LOW) for w in (w_qkv, w_qkv_far)]
    mixed_near, total_near = attend(info, qkv[0], quarter)
    mixed_far, total_far = attend(info, qkv[1], quarter)
    attention = scatter(
        lambda part: dot(mixed_near[part], w_out, 1, 0) + dot(mixed_far[part], w_out_far, 1, 0)
    )
    hidden = inputs + attention
    normed_ffn, factor_ffn = norm_rows(hidden, ffn_gain)
    rows_ffn = gather(normed_ffn)
    gates = jnp.concatenate((w_gate, w_gate_far), 1)
    ups = jnp.concatenate((w_up, w_up_far), 1)
    downs = jnp.concatenate((w_down, w_down_far), 0)
    gate_pre = dot(rows_ffn, gates, 1, 0, LOW).astype(F32)
    up_proj = dot(rows_ffn, ups, 1, 0, LOW).astype(F32)
    sigmoid = 1.0 / (1.0 + jnp.exp(-gate_pre))
    swish_gate = gate_pre * sigmoid
    product = (swish_gate * up_proj).astype(LOW)
    feedforward = scatter(lambda part: dot(product[part], downs, 1, 0))
    result = (live_rows * (hidden + feedforward)).astype(LOW)
    result_far = swap_chip(result[quarter:])
    output = jnp.where(
        chip == 0,
        jnp.stack((result[:quarter], result_far)),
        jnp.stack((result_far, result[:quarter])),
    )[:, None]

    grad_result = jnp.concatenate((cot_near, after(cot_far, rows_ffn)), 0).astype(F32) * live_rows
    grad_ffn = gather(grad_result.astype(LOW))
    grad_product = dot(grad_ffn, downs, 1, 1)
    grad_gate = (grad_product * up_proj * sigmoid * (1.0 + gate_pre * (1.0 - sigmoid))).astype(LOW)
    grad_up = (grad_product * swish_gate).astype(LOW)

    half = w_gate.shape[1]

    def over_chips(parts):
        far = swap_chip(jnp.concatenate([far.astype(LOW) for _, far in parts], 0))
        summed = jnp.concatenate([near for near, _ in parts], 0) + far.astype(F32)
        rows = summed.shape[0]
        held = summed.reshape(rows, groups, width // groups).transpose(1, 0, 2)
        step = 1
        while step < groups:
            side = (group // step) % 2
            pairs = held.reshape(-1, 2, rows, width // groups)
            moved = lax.ppermute(
                lax.dynamic_index_in_dim(pairs, 1 - side, 1, False).astype(LOW),
                "dp",
                [(i, i ^ step) for i in range(groups)],
            )
            held = lax.dynamic_index_in_dim(pairs, side, 1, False) + moved.astype(F32)
            step *= 2
        return held[0]

    def halves(value):
        return (value[:half], value[half:])

    down_shard = over_chips([halves(dot(product, grad_ffn, 0, 0))])
    up_halves = halves(dot(grad_up, rows_ffn, 0, 0))
    gate_up_shards = over_chips([halves(dot(grad_gate, rows_ffn, 0, 0)), up_halves])
    grad_normed_ffn = scatter(
        lambda part: dot(grad_gate[part], gates, 1, 1) + dot(grad_up[part], ups, 1, 1)
    )
    grad_hidden, gain_ffn_part = norm_back(hidden, factor_ffn, ffn_gain, grad_normed_ffn)
    grad_hidden = grad_hidden + grad_result
    grad_attn = gather(grad_hidden.astype(LOW))
    out_halves = (dot(mixed_near, grad_attn, 0, 0), dot(mixed_far, grad_attn, 0, 0))
    back_far = dot(grad_attn, w_out_far, 1, 1, LOW)
    grad_far = attend_back(info, qkv[1], back_far, mixed_far, total_far, quarter)
    grad_far = jnp.concatenate(grad_far, 1)
    weight_far = dot(grad_far, rows_attn, 0, 0, LOW)
    back_near = after(dot(grad_attn, w_out, 1, 1, LOW), weight_far)
    grad_near = attend_back(info, qkv[0], back_near, mixed_near, total_near, quarter)
    grad_near = jnp.concatenate(grad_near, 1)
    grad_normed_attn = scatter(
        lambda part: dot(grad_near[part], w_qkv, 1, 1) + dot(grad_far[part], w_qkv_far, 1, 1)
    )
    qkv_shards = over_chips([out_halves, (dot(grad_near, rows_attn, 0, 0), weight_far)])
    grad_inputs, gain_attn_part = norm_back(inputs, factor_attn, attn_gain, grad_normed_attn)
    grad_inputs = (grad_inputs + grad_hidden).astype(LOW)
    returned = exchange(grad_inputs[quarter:].reshape(groups, band, width))
    by_far = swap_chip(returned)
    by_near = exchange(grad_inputs[:quarter].reshape(groups, band, width))
    by_slot = jnp.where(
        chip == 0, jnp.stack((by_near, by_far), 1), jnp.stack((by_far, by_near), 1)
    ).reshape(seq_total, band, width)
    grad_patches = by_slot[deal][:, None]

    def total_of(value):
        value = value + swap_core(value)
        value = value + swap_chip(value)
        step = 1
        while step < groups:
            value = value + lax.ppermute(value, "dp", [(i, i ^ step) for i in range(groups)])
            step *= 2
        return value

    gain_grads = total_of(jnp.stack((gain_attn_part, gain_ffn_part)))
    part = w_query.shape[1]
    return (
        output,
        grad_patches,
        gain_grads[0],
        qkv_shards[part : 2 * part].T,
        qkv_shards[2 * part : 3 * part].T,
        qkv_shards[3 * part :].T,
        qkv_shards[:part],
        gain_grads[1],
        gate_up_shards[:half].T,
        gate_up_shards[half:].T,
        down_shard,
    )


def solution(mesh):
    in_specs = (
        P(None, "tensor", "dp", None),
        P(),
        P(),
        P(),
        P(None, "tensor"),
        P(None, "tensor"),
        P(None, "tensor"),
        P("tensor", None),
        P(),
        P(None, "tensor"),
        P(None, "tensor"),
        P("tensor", None),
        P("dp", "tensor", None, None),
    )
    out_specs = (
        P("dp", "tensor", None, None),
        P(None, "tensor", "dp", None),
        P(),
        P("dp", "tensor"),
        P("dp", "tensor"),
        P("dp", "tensor"),
        P("tensor", "dp"),
        P(),
        P("dp", "tensor"),
        P("dp", "tensor"),
        P("tensor", "dp"),
    )
    return jax.shard_map(layer, mesh=mesh, in_specs=in_specs, out_specs=out_specs, check_vma=False)
```

```python
import functools

import jax
import jax.numpy as jnp
from jax import lax
from jax.experimental import pallas as pl
from jax.experimental.pallas import tpu as pltpu
from jax.sharding import PartitionSpec as P


HEAD_DIM = 64
PAIR = 2 * HEAD_DIM
EPSILON = 1e-05
NEGATIVE = -1e30
LOW = jnp.bfloat16
F32 = jnp.float32


def dot(left, right, left_dim, right_dim, dtype=F32):
    return lax.dot_general(
        left, right, (((left_dim,), (right_dim,)), ((), ())), preferred_element_type=dtype
    )


def norm_rows(rows, gain_vector):
    factor = lax.rsqrt(jnp.mean(rows * rows, -1, keepdims=True) + EPSILON)
    return ((rows * factor * gain_vector).astype(LOW), factor)


def norm_back(rows, factor, gain_vector, upstream):
    scaled = upstream * gain_vector
    inward = factor * scaled - rows * factor**3 * jnp.mean(rows * scaled, -1, keepdims=True)
    return (inward, jnp.sum(upstream * rows * factor, 0))


def head_masks(rows):
    lane = lax.broadcasted_iota(jnp.int32, (rows, PAIR), 1)
    return (lane < HEAD_DIM, lane >= HEAD_DIM)


def attend_kernel(info, q_ref, k_ref, v_ref, o_ref, total_ref):
    block = q_ref.shape[0]
    number = pl.program_id(1)
    masks = head_masks(block)

    @pl.when(number < info[0])
    def _():
        query = q_ref[...] * jnp.asarray(HEAD_DIM**-0.5, LOW)
        queries = [jnp.where(m, query, jnp.zeros_like(query)) for m in masks]
        above = lax.broadcasted_iota(jnp.int32, (block, block), 0) >= lax.broadcasted_iota(
            jnp.int32, (block, block), 1
        )

        def step(key_number, state, diagonal):
            start = pl.multiple_of(info[1 + key_number] * block, block)
            keys = k_ref[pl.ds(start, block), :]
            values = v_ref[pl.ds(start, block), :]
            result = []
            for head in range(2):
                high, acc = state[head]
                scores = dot(queries[head], keys, 1, 1)
                if diagonal:
                    scores = jnp.where(above, scores, NEGATIVE)
                new_high = jnp.maximum(high, jnp.max(scores, -1, keepdims=True))
                probs = jnp.exp(scores - new_high).astype(LOW)
                extended = jnp.where(masks[head], values, jnp.ones_like(values))
                acc = acc * jnp.exp(high - new_high) + dot(probs, extended, 1, 0)
                result.append((new_high, acc))
            return tuple(result)

        start_state = tuple(
            (jnp.full((block, 1), NEGATIVE, F32), jnp.zeros((block, PAIR), F32)) for _ in range(2)
        )
        state = step(number, start_state, True)
        state = lax.fori_loop(0, number, lambda n, s: step(n, s, False), state)
        (high0, acc0), (high1, acc1) = state
        sum0 = acc0[:, HEAD_DIM : HEAD_DIM + 1]
        sum1 = acc1[:, 0:1]
        o_ref[...] = jnp.where(masks[0], acc0 / sum0, acc1 / sum1).astype(LOW)
        total_ref[...] = jnp.where(masks[0], high0 + jnp.log(sum0), high1 + jnp.log(sum1))

    @pl.when(number >= info[0])
    def _():
        o_ref[...] = jnp.zeros_like(o_ref)
        total_ref[...] = jnp.zeros_like(total_ref)


def attend(info, qkv, block):
    rows, width = qkv.shape
    pairs = width // (3 * PAIR)
    here = pl.BlockSpec((block, PAIR), lambda h, i, info: (info[1 + i], h))
    return pl.pallas_call(
        attend_kernel,
        grid_spec=pltpu.PrefetchScalarGridSpec(
            num_scalar_prefetch=1,
            grid=(pairs, rows // block),
            in_specs=[
                here,
                pl.BlockSpec((rows, PAIR), lambda h, i, info: (0, pairs + h)),
                pl.BlockSpec((rows, PAIR), lambda h, i, info: (0, 2 * pairs + h)),
            ],
            out_specs=[here, here],
        ),
        out_shape=[
            jax.ShapeDtypeStruct((rows, pairs * PAIR), LOW),
            jax.ShapeDtypeStruct((rows, pairs * PAIR), F32),
        ],
        name="attend",
    )(info, qkv, qkv, qkv)


def attend_back_kernel(
    block, info, q_ref, k_ref, v_ref, do_ref, o_ref, total_ref, dq_ref, dk_ref, dv_ref, dq_acc, dk_acc, dv_acc
):
    masks = head_masks(block)
    dk_acc[...] = jnp.zeros_like(dk_acc)
    dv_acc[...] = jnp.zeros_like(dv_acc)
    dq_ref[...] = jnp.zeros_like(dq_ref)
    below = lax.broadcasted_iota(jnp.int32, (block, block), 0) <= lax.broadcasted_iota(
        jnp.int32, (block, block), 1
    )

    def split(value):
        return [jnp.where(m, value, jnp.zeros_like(value)) for m in masks]

    def query_step(number, carry):
        start = pl.multiple_of(info[1 + number] * block, block)
        here = pl.ds(start, block)
        queries = split(q_ref[here, :] * jnp.asarray(HEAD_DIM**-0.5, LOW))
        grad = do_ref[here, :]
        grads = split(grad)
        product = (grad.astype(F32) * o_ref[here, :].astype(F32)).T
        row_dots = [
            jnp.sum(product[h * HEAD_DIM : (h + 1) * HEAD_DIM], 0, keepdims=True) for h in range(2)
        ]
        turned = total_ref[here, :].T
        totals = [turned[h * HEAD_DIM : h * HEAD_DIM + 1] for h in range(2)]
        dq_acc[...] = jnp.zeros_like(dq_acc)

        def key_step(key_number, diagonal):
            there = pl.ds(pl.multiple_of(info[1 + key_number] * block, block), block)
            keys = k_ref[there, :]
            values = v_ref[there, :]
            split_keys = split(keys)
            dq = dq_acc[...]
            dk = dk_acc[there, :]
            dv = dv_acc[there, :]
            for head in range(2):
                scores = dot(keys, queries[head], 1, 1)
                if diagonal:
                    scores = jnp.where(below, scores, NEGATIVE)
                probs = jnp.exp(scores - totals[head])
                grad_probs = dot(values, grads[head], 1, 1)
                grad_scores = (probs * (grad_probs - row_dots[head])).astype(LOW)
                dv = dv + dot(probs.astype(LOW), grads[head], 1, 0)
                dk = dk + dot(grad_scores, queries[head], 1, 0)
                dq = dq + dot(grad_scores, split_keys[head], 0, 0)
            dq_acc[...] = dq
            dk_acc[there, :] = dk
            dv_acc[there, :] = dv

        key_step(number, True)

        def loop_step(key_number, inner):
            key_step(key_number, False)
            return inner

        lax.fori_loop(0, number, loop_step, 0)
        dq_ref[here, :] = (dq_acc[...] * HEAD_DIM**-0.5).astype(LOW)
        return carry

    lax.fori_loop(0, info[0], query_step, 0)
    dk_ref[...] = dk_acc[...].astype(LOW)
    dv_ref[...] = dv_acc[...].astype(LOW)


def attend_back(info, qkv, grad_out, mixed, totals, block):
    rows, width = qkv.shape
    pairs = width // (3 * PAIR)

    def column(offset):
        return pl.BlockSpec((rows, PAIR), lambda h, info: (0, offset + h))

    shape = jax.ShapeDtypeStruct((rows, pairs * PAIR), LOW)
    return pl.pallas_call(
        functools.partial(attend_back_kernel, block),
        grid_spec=pltpu.PrefetchScalarGridSpec(
            num_scalar_prefetch=1,
            grid=(pairs,),
            in_specs=[column(0), column(pairs), column(2 * pairs), column(0), column(0), column(0)],
            out_specs=[column(0)] * 3,
            scratch_shapes=[
                pltpu.VMEM((block, PAIR), F32),
                pltpu.VMEM((rows, PAIR), F32),
                pltpu.VMEM((rows, PAIR), F32),
            ],
        ),
        out_shape=[shape] * 3,
        name="attend_back",
    )(info, qkv, qkv, qkv, grad_out, mixed, totals)


def after(value, *others):
    return lax.optimization_barrier((value,) + others)[0]


def layer(
    patches,
    lengths,
    deal,
    attn_gain,
    w_query,
    w_key,
    w_value,
    w_out,
    ffn_gain,
    w_gate,
    w_up,
    w_down,
    cotangent,
):
    groups = lax.axis_size("dp")
    seq_total = patches.shape[0]
    band = patches.shape[2]
    quarter = cotangent.shape[2]
    width = patches.shape[3]
    group = lax.axis_index("dp")
    place = lax.axis_index("tensor")
    chip = place // 2
    core = place % 2

    def swap_core(value):
        return lax.ppermute(value, "tensor", [(0, 1), (1, 0), (2, 3), (3, 2)])

    def swap_chip(value):
        return lax.ppermute(value, "tensor", [(0, 2), (2, 0), (1, 3), (3, 1)])

    def exchange(value):
        return lax.all_to_all(value, "dp", split_axis=0, concat_axis=0, tiled=True)

    slot_owner = jnp.argsort(deal)
    owners = slot_owner.reshape(groups, 2)
    mine = jnp.take(owners, chip, axis=1)
    theirs = jnp.take(owners, 1 - chip, axis=1)
    length = lengths[mine[group]]
    given = swap_chip(patches[theirs, 0])
    arrived_near = exchange(patches[mine, 0])
    arrived_far = exchange(given)
    inputs = jnp.stack((arrived_near, arrived_far)).reshape(2 * quarter, width).astype(F32)

    w_qkv = jnp.concatenate((w_query, w_key, w_value), 1)
    w_qkv_far = swap_chip(w_qkv)
    w_out_far = swap_chip(w_out)
    w_gate_far = swap_chip(w_gate)
    w_up_far = swap_chip(w_up)
    w_down_far = swap_chip(w_down)
    cot_near = jnp.take(cotangent[:, 0], chip, axis=0)
    cot_far = swap_chip(jnp.take(cotangent[:, 0], 1 - chip, axis=0))

    numbers = jnp.arange(4)
    slots = 2 * (numbers % 2 != core) + (numbers // 2 != chip)
    live_blocks = (length + quarter - 1) // quarter
    info = jnp.concatenate((live_blocks[None], slots)).astype(jnp.int32)
    offsets = jnp.arange(quarter)
    positions = jnp.concatenate(
        ((2 * chip + core) * quarter + offsets, (2 * (1 - chip) + core) * quarter + offsets)
    )
    live_rows = (positions < length).astype(F32)[:, None]
    own_rows = 2 * quarter

    def gather(value):
        other = swap_core(value)
        return jnp.concatenate((value, other), 0)

    def scatter(make):
        far = make(slice(own_rows, None)).astype(LOW)
        far = swap_core(far)
        return make(slice(0, own_rows)) + far.astype(F32)

    normed_attn, factor_attn = norm_rows(inputs, attn_gain)
    rows_attn = gather(normed_attn)
    qkv = [dot(rows_attn, w, 1, 0, LOW) for w in (w_qkv, w_qkv_far)]
    mixed_near, total_near = attend(info, qkv[0], quarter)
    mixed_far, total_far = attend(info, qkv[1], quarter)
    attention = scatter(
        lambda part: dot(mixed_near[part], w_out, 1, 0) + dot(mixed_far[part], w_out_far, 1, 0),
    )
    hidden = inputs + attention
    normed_ffn, factor_ffn = norm_rows(hidden, ffn_gain)
    rows_ffn = gather(normed_ffn)
    gates = jnp.concatenate((w_gate, w_gate_far), 1)
    ups = jnp.concatenate((w_up, w_up_far), 1)
    downs = jnp.concatenate((w_down, w_down_far), 0)
    gate_pre = dot(rows_ffn, gates, 1, 0, LOW).astype(F32)
    up_proj = dot(rows_ffn, ups, 1, 0, LOW).astype(F32)
    sigmoid = 1.0 / (1.0 + jnp.exp(-gate_pre))
    swish_gate = gate_pre * sigmoid
    product = (swish_gate * up_proj).astype(LOW)
    feedforward = scatter(lambda part: dot(product[part], downs, 1, 0))
    result = (live_rows * (hidden + feedforward)).astype(LOW)
    result_far = swap_chip(result[quarter:])
    output = jnp.where(
        chip == 0,
        jnp.stack((result[:quarter], result_far)),
        jnp.stack((result_far, result[:quarter])),
    )[:, None]

    grad_result = jnp.concatenate((cot_near, cot_far), 0).astype(F32) * live_rows
    grad_ffn = gather(grad_result.astype(LOW))
    grad_product = dot(grad_ffn, downs, 1, 1)
    grad_gate = (grad_product * up_proj * sigmoid * (1.0 + gate_pre * (1.0 - sigmoid))).astype(LOW)
    grad_up = (grad_product * swish_gate).astype(LOW)

    half = w_gate.shape[1]

    def over_chips(parts):
        far = swap_chip(jnp.concatenate([far.astype(LOW) for _, far in parts], 0))
        summed = jnp.concatenate([near for near, _ in parts], 0) + far.astype(F32)
        rows = summed.shape[0]
        held = summed.reshape(rows, groups, width // groups).transpose(1, 0, 2)
        step = 1
        while step < groups:
            side = (group // step) % 2
            pairs = held.reshape(-1, 2, rows, width // groups)
            moved = lax.ppermute(
                lax.dynamic_index_in_dim(pairs, 1 - side, 1, False).astype(LOW),
                "dp",
                [(i, i ^ step) for i in range(groups)],
            )
            held = lax.dynamic_index_in_dim(pairs, side, 1, False) + moved.astype(F32)
            step *= 2
        return held[0]

    def halves(value):
        return (value[:half], value[half:])

    down_shard = over_chips([halves(dot(product, grad_ffn, 0, 0))])
    up_halves = halves(dot(grad_up, rows_ffn, 0, 0))
    gate_up_shards = over_chips([halves(dot(grad_gate, rows_ffn, 0, 0)), up_halves])
    grad_normed_ffn = scatter(
        lambda part: dot(grad_gate[part], gates, 1, 1) + dot(grad_up[part], ups, 1, 1),
    )
    grad_hidden, gain_ffn_part = norm_back(hidden, factor_ffn, ffn_gain, grad_normed_ffn)
    grad_hidden = grad_hidden + grad_result
    grad_attn = gather(grad_hidden.astype(LOW))
    out_halves = (dot(mixed_near, grad_attn, 0, 0), dot(mixed_far, grad_attn, 0, 0))
    back_far = dot(grad_attn, w_out_far, 1, 1, LOW)
    grad_far = attend_back(info, qkv[1], back_far, mixed_far, total_far, quarter)
    grad_far = jnp.concatenate(grad_far, 1)
    weight_far = dot(grad_far, rows_attn, 0, 0, LOW)
    back_near = after(dot(grad_attn, w_out, 1, 1, LOW), weight_far)
    grad_near = attend_back(info, qkv[0], back_near, mixed_near, total_near, quarter)
    grad_near = jnp.concatenate(grad_near, 1)
    grad_normed_attn = scatter(
        lambda part: dot(grad_near[part], w_qkv, 1, 1) + dot(grad_far[part], w_qkv_far, 1, 1),
    )
    qkv_shards = over_chips([out_halves, (dot(grad_near, rows_attn, 0, 0), weight_far)])
    grad_inputs, gain_attn_part = norm_back(inputs, factor_attn, attn_gain, grad_normed_attn)
    grad_inputs = (grad_inputs + grad_hidden).astype(LOW)
    returned = exchange(grad_inputs[quarter:].reshape(groups, band, width))
    by_far = swap_chip(returned)
    by_near = exchange(grad_inputs[:quarter].reshape(groups, band, width))
    by_slot = jnp.where(
        chip == 0, jnp.stack((by_near, by_far), 1), jnp.stack((by_far, by_near), 1)
    ).reshape(seq_total, band, width)
    grad_patches = by_slot[deal][:, None]

    def total_of(value):
        value = value + swap_core(value)
        value = value + swap_chip(value)
        step = 1
        while step < groups:
            moved = lax.ppermute(value, "dp", [(i, i ^ step) for i in range(groups)])
            value = value + moved
            step *= 2
        return value

    gain_grads = total_of(jnp.stack((gain_attn_part, gain_ffn_part)))
    part = w_query.shape[1]
    return (
        output,
        grad_patches,
        gain_grads[0],
        qkv_shards[part : 2 * part].T,
        qkv_shards[2 * part : 3 * part].T,
        qkv_shards[3 * part :].T,
        qkv_shards[:part],
        gain_grads[1],
        gate_up_shards[:half].T,
        gate_up_shards[half:].T,
        down_shard,
    )


def solution(mesh):
    in_specs = (
        P(None, "tensor", "dp", None),
        P(),
        P(),
        P(),
        P(None, "tensor"),
        P(None, "tensor"),
        P(None, "tensor"),
        P("tensor", None),
        P(),
        P(None, "tensor"),
        P(None, "tensor"),
        P("tensor", None),
        P("dp", "tensor", None, None),
    )
    out_specs = (
        P("dp", "tensor", None, None),
        P(None, "tensor", "dp", None),
        P(),
        P("dp", "tensor"),
        P("dp", "tensor"),
        P("dp", "tensor"),
        P("tensor", "dp"),
        P(),
        P("dp", "tensor"),
        P("dp", "tensor"),
        P("tensor", "dp"),
    )
    return jax.shard_map(layer, mesh=mesh, in_specs=in_specs, out_specs=out_specs, check_vma=False)
```

```python
import functools

import jax
import jax.numpy as jnp
from jax import lax
from jax.experimental import pallas as pl
from jax.experimental.pallas import tpu as pltpu
from jax.sharding import PartitionSpec as P


HEAD_DIM = 64
PAIR = 2 * HEAD_DIM
EPSILON = 1e-05
NEGATIVE = -1e30
LOW = jnp.bfloat16
F32 = jnp.float32


def dot(left, right, left_dim, right_dim, dtype=F32):
    return lax.dot_general(
        left, right, (((left_dim,), (right_dim,)), ((), ())), preferred_element_type=dtype
    )


def norm_rows(rows, gain_vector):
    factor = lax.rsqrt(jnp.mean(rows * rows, -1, keepdims=True) + EPSILON)
    return ((rows * factor * gain_vector).astype(LOW), factor)


def norm_back(rows, factor, gain_vector, upstream):
    scaled = upstream * gain_vector
    inward = factor * scaled - rows * factor**3 * jnp.mean(rows * scaled, -1, keepdims=True)
    return (inward, jnp.sum(upstream * rows * factor, 0))


def head_masks(rows):
    lane = lax.broadcasted_iota(jnp.int32, (rows, PAIR), 1)
    return (lane < HEAD_DIM, lane >= HEAD_DIM)


def attend_kernel(info, q_ref, k_ref, v_ref, o_ref, total_ref):
    block = q_ref.shape[0]
    number = pl.program_id(1)
    masks = head_masks(block)

    @pl.when(number < info[0])
    def _():
        query = q_ref[...] * jnp.asarray(HEAD_DIM**-0.5, LOW)
        queries = [jnp.where(m, query, jnp.zeros_like(query)) for m in masks]
        below = lax.broadcasted_iota(jnp.int32, (block, block), 0) <= lax.broadcasted_iota(
            jnp.int32, (block, block), 1
        )

        def step(key_number, state, diagonal):
            start = pl.multiple_of(info[1 + key_number] * block, block)
            keys = k_ref[pl.ds(start, block), :]
            values = v_ref[pl.ds(start, block), :]
            result = []
            for head in range(2):
                high, acc = state[head]
                scores = dot(keys, queries[head], 1, 1)
                if diagonal:
                    scores = jnp.where(below, scores, NEGATIVE)
                new_high = jnp.maximum(high, jnp.max(scores, 0, keepdims=True))
                probs = jnp.exp(scores - new_high).astype(LOW)
                extended = jnp.where(masks[head], values, jnp.ones_like(values))
                acc = acc * jnp.exp(high - new_high) + dot(extended, probs, 0, 0)
                result.append((new_high, acc))
            return tuple(result)

        start_state = tuple(
            (jnp.full((1, block), NEGATIVE, F32), jnp.zeros((PAIR, block), F32)) for _ in range(2)
        )
        state = step(number, start_state, True)
        state = lax.fori_loop(0, number, lambda n, s: step(n, s, False), state)
        (high0, acc0), (high1, acc1) = state
        sum0 = acc0[HEAD_DIM : HEAD_DIM + 1]
        sum1 = acc1[0:1]
        mixed = jnp.concatenate((acc0[:HEAD_DIM] / sum0, acc1[HEAD_DIM:] / sum1), 0)
        o_ref[...] = mixed.T.astype(LOW)
        first = lax.broadcasted_iota(jnp.int32, (PAIR, block), 0) < HEAD_DIM
        total_ref[...] = jnp.where(first, high0 + jnp.log(sum0), high1 + jnp.log(sum1)).T

    @pl.when(number >= info[0])
    def _():
        o_ref[...] = jnp.zeros_like(o_ref)
        total_ref[...] = jnp.zeros_like(total_ref)


def attend(info, qkv, block):
    rows, width = qkv.shape
    pairs = width // (3 * PAIR)
    here = pl.BlockSpec((block, PAIR), lambda h, i, info: (info[1 + i], h))
    return pl.pallas_call(
        attend_kernel,
        grid_spec=pltpu.PrefetchScalarGridSpec(
            num_scalar_prefetch=1,
            grid=(pairs, rows // block),
            in_specs=[
                here,
                pl.BlockSpec((rows, PAIR), lambda h, i, info: (0, pairs + h)),
                pl.BlockSpec((rows, PAIR), lambda h, i, info: (0, 2 * pairs + h)),
            ],
            out_specs=[here, here],
        ),
        out_shape=[
            jax.ShapeDtypeStruct((rows, pairs * PAIR), LOW),
            jax.ShapeDtypeStruct((rows, pairs * PAIR), F32),
        ],
        name="attend",
    )(info, qkv, qkv, qkv)


def attend_back_kernel(
    block, info, q_ref, k_ref, v_ref, do_ref, o_ref, total_ref, dq_ref, dk_ref, dv_ref, dq_acc, dk_acc, dv_acc
):
    masks = head_masks(block)
    dk_acc[...] = jnp.zeros_like(dk_acc)
    dv_acc[...] = jnp.zeros_like(dv_acc)
    dq_ref[...] = jnp.zeros_like(dq_ref)
    below = lax.broadcasted_iota(jnp.int32, (block, block), 0) <= lax.broadcasted_iota(
        jnp.int32, (block, block), 1
    )

    def split(value):
        return [jnp.where(m, value, jnp.zeros_like(value)) for m in masks]

    def query_step(number, carry):
        start = pl.multiple_of(info[1 + number] * block, block)
        here = pl.ds(start, block)
        queries = split(q_ref[here, :] * jnp.asarray(HEAD_DIM**-0.5, LOW))
        grad = do_ref[here, :]
        grads = split(grad)
        product = (grad.astype(F32) * o_ref[here, :].astype(F32)).T
        row_dots = [
            jnp.sum(product[h * HEAD_DIM : (h + 1) * HEAD_DIM], 0, keepdims=True) for h in range(2)
        ]
        turned = total_ref[here, :].T
        totals = [turned[h * HEAD_DIM : h * HEAD_DIM + 1] for h in range(2)]
        dq_acc[...] = jnp.zeros_like(dq_acc)

        def key_step(key_number, diagonal):
            there = pl.ds(pl.multiple_of(info[1 + key_number] * block, block), block)
            keys = k_ref[there, :]
            values = v_ref[there, :]
            split_keys = split(keys)
            dq = dq_acc[...]
            dk = dk_acc[there, :]
            dv = dv_acc[there, :]
            for head in range(2):
                scores = dot(keys, queries[head], 1, 1)
                if diagonal:
                    scores = jnp.where(below, scores, NEGATIVE)
                probs = jnp.exp(scores - totals[head])
                grad_probs = dot(values, grads[head], 1, 1)
                grad_scores = (probs * (grad_probs - row_dots[head])).astype(LOW)
                dv = dv + dot(probs.astype(LOW), grads[head], 1, 0)
                dk = dk + dot(grad_scores, queries[head], 1, 0)
                dq = dq + dot(grad_scores, split_keys[head], 0, 0)
            dq_acc[...] = dq
            dk_acc[there, :] = dk
            dv_acc[there, :] = dv

        key_step(number, True)

        def loop_step(key_number, inner):
            key_step(key_number, False)
            return inner

        lax.fori_loop(0, number, loop_step, 0)
        dq_ref[here, :] = (dq_acc[...] * HEAD_DIM**-0.5).astype(LOW)
        return carry

    lax.fori_loop(0, info[0], query_step, 0)
    dk_ref[...] = dk_acc[...].astype(LOW)
    dv_ref[...] = dv_acc[...].astype(LOW)


def attend_back(info, qkv, grad_out, mixed, totals, block, first, count):
    rows, width = qkv.shape
    pairs = width // (3 * PAIR)

    def column(offset):
        return pl.BlockSpec((rows, PAIR), lambda h, info: (0, offset + first + h))

    given = pl.BlockSpec((rows, PAIR), lambda h, info: (0, h))
    shape = jax.ShapeDtypeStruct((rows, count * PAIR), LOW)
    return pl.pallas_call(
        functools.partial(attend_back_kernel, block),
        grid_spec=pltpu.PrefetchScalarGridSpec(
            num_scalar_prefetch=1,
            grid=(count,),
            in_specs=[column(0), column(pairs), column(2 * pairs), column(0), column(0), column(0)],
            out_specs=[given] * 3,
            scratch_shapes=[
                pltpu.VMEM((block, PAIR), F32),
                pltpu.VMEM((rows, PAIR), F32),
                pltpu.VMEM((rows, PAIR), F32),
            ],
        ),
        out_shape=[shape] * 3,
        name="attend_back",
    )(info, qkv, qkv, qkv, grad_out, mixed, totals)


def after(value, *others):
    return lax.optimization_barrier((value,) + others)[0]


def layer(
    patches,
    lengths,
    deal,
    attn_gain,
    w_query,
    w_key,
    w_value,
    w_out,
    ffn_gain,
    w_gate,
    w_up,
    w_down,
    cotangent,
):
    groups = lax.axis_size("dp")
    seq_total = patches.shape[0]
    band = patches.shape[2]
    quarter = cotangent.shape[2]
    width = patches.shape[3]
    group = lax.axis_index("dp")
    place = lax.axis_index("tensor")
    chip = place // 2
    core = place % 2

    def swap_core(value):
        return lax.ppermute(value, "tensor", [(0, 1), (1, 0), (2, 3), (3, 2)])

    def swap_chip(value):
        return lax.ppermute(value, "tensor", [(0, 2), (2, 0), (1, 3), (3, 1)])

    def exchange(value):
        return lax.all_to_all(value, "dp", split_axis=0, concat_axis=0, tiled=True)

    slot_owner = jnp.argsort(deal)
    owners = slot_owner.reshape(groups, 2)
    mine = jnp.take(owners, chip, axis=1)
    theirs = jnp.take(owners, 1 - chip, axis=1)
    length = lengths[mine[group]]
    given = swap_chip(patches[theirs, 0])
    arrived_near = exchange(patches[mine, 0])
    arrived_far = exchange(given)
    inputs = jnp.stack((arrived_near, arrived_far)).reshape(2 * quarter, width).astype(F32)

    w_qkv = jnp.concatenate((w_query, w_key, w_value), 1)
    w_qkv_far = swap_chip(w_qkv)
    w_out_far = swap_chip(w_out)
    w_gate_far = swap_chip(w_gate)
    w_up_far = swap_chip(w_up)
    w_down_far = swap_chip(w_down)
    cot_near = jnp.take(cotangent[:, 0], chip, axis=0)
    cot_far = swap_chip(jnp.take(cotangent[:, 0], 1 - chip, axis=0))

    numbers = jnp.arange(4)
    slots = 2 * (numbers % 2 != core) + (numbers // 2 != chip)
    live_blocks = (length + quarter - 1) // quarter
    info = jnp.concatenate((live_blocks[None], slots)).astype(jnp.int32)
    offsets = jnp.arange(quarter)
    positions = jnp.concatenate(
        ((2 * chip + core) * quarter + offsets, (2 * (1 - chip) + core) * quarter + offsets)
    )
    live_rows = (positions < length).astype(F32)[:, None]
    own_rows = 2 * quarter

    def gather(value):
        other = swap_core(value)
        return jnp.concatenate((value, other), 0)

    def scatter(make):
        far = make(slice(own_rows, None)).astype(LOW)
        far = swap_core(far)
        return make(slice(0, own_rows)) + far.astype(F32)

    normed_attn, factor_attn = norm_rows(inputs, attn_gain)
    rows_attn = gather(normed_attn)
    qkv = [dot(rows_attn, w, 1, 0, LOW) for w in (w_qkv, w_qkv_far)]
    mixed_near, total_near = attend(info, qkv[0], quarter)
    mixed_far, total_far = attend(info, qkv[1], quarter)
    attention = scatter(
        lambda part: dot(mixed_near[part], w_out, 1, 0) + dot(mixed_far[part], w_out_far, 1, 0),
    )
    hidden = inputs + attention
    normed_ffn, factor_ffn = norm_rows(hidden, ffn_gain)
    rows_ffn = gather(normed_ffn)
    gates = jnp.concatenate((w_gate, w_gate_far), 1)
    ups = jnp.concatenate((w_up, w_up_far), 1)
    downs = jnp.concatenate((w_down, w_down_far), 0)
    gate_pre = dot(rows_ffn, gates, 1, 0, LOW).astype(F32)
    up_proj = dot(rows_ffn, ups, 1, 0, LOW).astype(F32)
    sigmoid = 1.0 / (1.0 + jnp.exp(-gate_pre))
    swish_gate = gate_pre * sigmoid
    product = (swish_gate * up_proj).astype(LOW)
    feedforward = scatter(lambda part: dot(product[part], downs, 1, 0))
    result = (live_rows * (hidden + feedforward)).astype(LOW)
    result_far = swap_chip(result[quarter:])
    output = jnp.where(
        chip == 0,
        jnp.stack((result[:quarter], result_far)),
        jnp.stack((result_far, result[:quarter])),
    )[:, None]

    grad_result = jnp.concatenate((cot_near, cot_far), 0).astype(F32) * live_rows
    grad_ffn = gather(grad_result.astype(LOW))
    grad_product = dot(grad_ffn, downs, 1, 1)
    grad_gate = (grad_product * up_proj * sigmoid * (1.0 + gate_pre * (1.0 - sigmoid))).astype(LOW)
    grad_up = (grad_product * swish_gate).astype(LOW)

    half = w_gate.shape[1]

    def over_chips(parts):
        far = swap_chip(jnp.concatenate([far.astype(LOW) for _, far in parts], 0))
        summed = jnp.concatenate([near for near, _ in parts], 0) + far.astype(F32)
        rows = summed.shape[0]
        held = summed.reshape(rows, groups, width // groups).transpose(1, 0, 2)
        step = 1
        while step < groups:
            side = (group // step) % 2
            pairs = held.reshape(-1, 2, rows, width // groups)
            moved = lax.ppermute(
                lax.dynamic_index_in_dim(pairs, 1 - side, 1, False).astype(LOW),
                "dp",
                [(i, i ^ step) for i in range(groups)],
            )
            held = lax.dynamic_index_in_dim(pairs, side, 1, False) + moved.astype(F32)
            step *= 2
        return held[0]

    def halves(value):
        return (value[:half], value[half:])

    down_shard = over_chips([halves(dot(product, grad_ffn, 0, 0))])
    up_halves = halves(dot(grad_up, rows_ffn, 0, 0))
    gate_up_shards = over_chips([halves(dot(grad_gate, rows_ffn, 0, 0)), up_halves])
    grad_normed_ffn = scatter(
        lambda part: dot(grad_gate[part], gates, 1, 1) + dot(grad_up[part], ups, 1, 1),
    )
    grad_hidden, gain_ffn_part = norm_back(hidden, factor_ffn, ffn_gain, grad_normed_ffn)
    grad_hidden = grad_hidden + grad_result
    grad_attn = gather(grad_hidden.astype(LOW))
    out_halves = (dot(mixed_near, grad_attn, 0, 0), dot(mixed_far, grad_attn, 0, 0))
    back_far = dot(grad_attn, w_out_far, 1, 1, LOW)
    grad_far = attend_back(
        info, qkv[1], back_far, mixed_far, total_far, quarter, 0, mixed_far.shape[1] // PAIR
    )
    grad_far = jnp.concatenate(grad_far, 1)
    weight_far = dot(grad_far, rows_attn, 0, 0, LOW)
    back_near = after(dot(grad_attn, w_out, 1, 1, LOW), weight_far)
    near_pairs = mixed_near.shape[1] // PAIR
    first_near = attend_back(
        info, qkv[0], back_near, mixed_near, total_near, quarter, 0, near_pairs // 2
    )
    last_near = attend_back(
        info, qkv[0], back_near, mixed_near, total_near, quarter, near_pairs // 2, near_pairs // 2
    )
    grad_near = jnp.concatenate(
        [part for both in zip(first_near, last_near) for part in both], 1
    )
    grad_normed_attn = scatter(
        lambda part: dot(grad_near[part], w_qkv, 1, 1) + dot(grad_far[part], w_qkv_far, 1, 1),
    )
    qkv_shards = over_chips([out_halves, (dot(grad_near, rows_attn, 0, 0), weight_far)])
    grad_inputs, gain_attn_part = norm_back(inputs, factor_attn, attn_gain, grad_normed_attn)
    grad_inputs = (grad_inputs + grad_hidden).astype(LOW)
    returned = exchange(grad_inputs[quarter:].reshape(groups, band, width))
    by_far = swap_chip(returned)
    by_near = exchange(grad_inputs[:quarter].reshape(groups, band, width))
    by_slot = jnp.where(
        chip == 0, jnp.stack((by_near, by_far), 1), jnp.stack((by_far, by_near), 1)
    ).reshape(seq_total, band, width)
    grad_patches = by_slot[deal][:, None]

    def total_of(value):
        value = value + swap_core(value)
        value = value + swap_chip(value)
        step = 1
        while step < groups:
            moved = lax.ppermute(value, "dp", [(i, i ^ step) for i in range(groups)])
            value = value + moved
            step *= 2
        return value

    gain_grads = total_of(jnp.stack((gain_attn_part, gain_ffn_part)))
    part = w_query.shape[1]
    return (
        output,
        grad_patches,
        gain_grads[0],
        qkv_shards[part : 2 * part].T,
        qkv_shards[2 * part : 3 * part].T,
        qkv_shards[3 * part :].T,
        qkv_shards[:part],
        gain_grads[1],
        gate_up_shards[:half].T,
        gate_up_shards[half:].T,
        down_shard,
    )


def solution(mesh):
    in_specs = (
        P(None, "tensor", "dp", None),
        P(),
        P(),
        P(),
        P(None, "tensor"),
        P(None, "tensor"),
        P(None, "tensor"),
        P("tensor", None),
        P(),
        P(None, "tensor"),
        P(None, "tensor"),
        P("tensor", None),
        P("dp", "tensor", None, None),
    )
    out_specs = (
        P("dp", "tensor", None, None),
        P(None, "tensor", "dp", None),
        P(),
        P("dp", "tensor"),
        P("dp", "tensor"),
        P("dp", "tensor"),
        P("tensor", "dp"),
        P(),
        P("dp", "tensor"),
        P("dp", "tensor"),
        P("tensor", "dp"),
    )
    return jax.shard_map(layer, mesh=mesh, in_specs=in_specs, out_specs=out_specs, check_vma=False)
```

```python
import functools

import jax
import jax.numpy as jnp
from jax import lax
from jax.experimental import pallas as pl
from jax.experimental.pallas import tpu as pltpu
from jax.sharding import PartitionSpec as P


HEAD_DIM = 64
PAIR = 2 * HEAD_DIM
EPSILON = 1e-05
NEGATIVE = -1e30
LOW = jnp.bfloat16
F32 = jnp.float32


def dot(left, right, left_dim, right_dim, dtype=F32):
    return lax.dot_general(
        left, right, (((left_dim,), (right_dim,)), ((), ())), preferred_element_type=dtype
    )


def norm_rows(rows, gain_vector):
    factor = lax.rsqrt(jnp.mean(rows * rows, -1, keepdims=True) + EPSILON)
    return ((rows * factor * gain_vector).astype(LOW), factor)


def norm_back(rows, factor, gain_vector, upstream):
    scaled = upstream * gain_vector
    inward = factor * scaled - rows * factor**3 * jnp.mean(rows * scaled, -1, keepdims=True)
    return (inward, jnp.sum(upstream * rows * factor, 0))


def head_masks(rows):
    lane = lax.broadcasted_iota(jnp.int32, (rows, PAIR), 1)
    return (lane < HEAD_DIM, lane >= HEAD_DIM)


def attend_kernel(info, q_ref, k_ref, v_ref, o_ref, total_ref):
    block = q_ref.shape[0]
    number = pl.program_id(1)
    masks = head_masks(block)

    @pl.when(number < info[0])
    def _():
        query = q_ref[...] * jnp.asarray(HEAD_DIM**-0.5, LOW)
        queries = [jnp.where(m, query, jnp.zeros_like(query)) for m in masks]
        below = lax.broadcasted_iota(jnp.int32, (block, block), 0) <= lax.broadcasted_iota(
            jnp.int32, (block, block), 1
        )

        def step(key_number, state, diagonal):
            start = pl.multiple_of(info[1 + key_number] * block, block)
            keys = k_ref[pl.ds(start, block), :]
            values = v_ref[pl.ds(start, block), :]
            result = []
            for head in range(2):
                high, acc = state[head]
                scores = dot(keys, queries[head], 1, 1)
                if diagonal:
                    scores = jnp.where(below, scores, NEGATIVE)
                new_high = jnp.maximum(high, jnp.max(scores, 0, keepdims=True))
                probs = jnp.exp(scores - new_high).astype(LOW)
                extended = jnp.where(masks[head], values, jnp.ones_like(values))
                acc = acc * jnp.exp(high - new_high) + dot(extended, probs, 0, 0)
                result.append((new_high, acc))
            return tuple(result)

        start_state = tuple(
            (jnp.full((1, block), NEGATIVE, F32), jnp.zeros((PAIR, block), F32)) for _ in range(2)
        )
        state = step(number, start_state, True)
        state = lax.fori_loop(0, number, lambda n, s: step(n, s, False), state)
        (high0, acc0), (high1, acc1) = state
        sum0 = acc0[HEAD_DIM : HEAD_DIM + 1]
        sum1 = acc1[0:1]
        mixed = jnp.concatenate((acc0[:HEAD_DIM] / sum0, acc1[HEAD_DIM:] / sum1), 0)
        o_ref[...] = mixed.T.astype(LOW)
        first = lax.broadcasted_iota(jnp.int32, (PAIR, block), 0) < HEAD_DIM
        total_ref[...] = jnp.where(first, high0 + jnp.log(sum0), high1 + jnp.log(sum1)).T

    @pl.when(number >= info[0])
    def _():
        o_ref[...] = jnp.zeros_like(o_ref)
        total_ref[...] = jnp.zeros_like(total_ref)


def attend(info, qkv, block):
    rows, width = qkv.shape
    pairs = width // (3 * PAIR)
    here = pl.BlockSpec((block, PAIR), lambda h, i, info: (info[1 + i], h))
    return pl.pallas_call(
        attend_kernel,
        grid_spec=pltpu.PrefetchScalarGridSpec(
            num_scalar_prefetch=1,
            grid=(pairs, rows // block),
            in_specs=[
                here,
                pl.BlockSpec((rows, PAIR), lambda h, i, info: (0, pairs + h)),
                pl.BlockSpec((rows, PAIR), lambda h, i, info: (0, 2 * pairs + h)),
            ],
            out_specs=[here, here],
        ),
        out_shape=[
            jax.ShapeDtypeStruct((rows, pairs * PAIR), LOW),
            jax.ShapeDtypeStruct((rows, pairs * PAIR), F32),
        ],
        name="attend",
    )(info, qkv, qkv, qkv)


def attend_back_kernel(
    block, info, q_ref, k_ref, v_ref, do_ref, o_ref, total_ref, dq_ref, dk_ref, dv_ref, dq_acc, dk_acc, dv_acc
):
    masks = head_masks(block)
    dk_acc[...] = jnp.zeros_like(dk_acc)
    dv_acc[...] = jnp.zeros_like(dv_acc)
    dq_ref[...] = jnp.zeros_like(dq_ref)
    below = lax.broadcasted_iota(jnp.int32, (block, block), 0) <= lax.broadcasted_iota(
        jnp.int32, (block, block), 1
    )

    def split(value):
        return [jnp.where(m, value, jnp.zeros_like(value)) for m in masks]

    def query_step(number, carry):
        start = pl.multiple_of(info[1 + number] * block, block)
        here = pl.ds(start, block)
        queries = split(q_ref[here, :] * jnp.asarray(HEAD_DIM**-0.5, LOW))
        grad = do_ref[here, :]
        grads = split(grad)
        product = (grad.astype(F32) * o_ref[here, :].astype(F32)).T
        row_dots = [
            jnp.sum(product[h * HEAD_DIM : (h + 1) * HEAD_DIM], 0, keepdims=True) for h in range(2)
        ]
        turned = total_ref[here, :].T
        totals = [turned[h * HEAD_DIM : h * HEAD_DIM + 1] for h in range(2)]
        dq_acc[...] = jnp.zeros_like(dq_acc)

        def key_step(key_number, diagonal):
            there = pl.ds(pl.multiple_of(info[1 + key_number] * block, block), block)
            keys = k_ref[there, :]
            values = v_ref[there, :]
            split_keys = split(keys)
            dq = dq_acc[...]
            dk = dk_acc[there, :]
            dv = dv_acc[there, :]
            for head in range(2):
                scores = dot(keys, queries[head], 1, 1)
                if diagonal:
                    scores = jnp.where(below, scores, NEGATIVE)
                probs = jnp.exp(scores - totals[head])
                grad_probs = dot(values, grads[head], 1, 1)
                grad_scores = (probs * (grad_probs - row_dots[head])).astype(LOW)
                dv = dv + dot(probs.astype(LOW), grads[head], 1, 0)
                dk = dk + dot(grad_scores, queries[head], 1, 0)
                dq = dq + dot(grad_scores, split_keys[head], 0, 0)
            dq_acc[...] = dq
            dk_acc[there, :] = dk
            dv_acc[there, :] = dv

        key_step(number, True)

        def loop_step(key_number, inner):
            key_step(key_number, False)
            return inner

        lax.fori_loop(0, number, loop_step, 0)
        dq_ref[here, :] = (dq_acc[...] * HEAD_DIM**-0.5).astype(LOW)
        return carry

    lax.fori_loop(0, info[0], query_step, 0)
    dk_ref[...] = dk_acc[...].astype(LOW)
    dv_ref[...] = dv_acc[...].astype(LOW)


def attend_back(info, qkv, grad_out, mixed, totals, block):
    rows, width = qkv.shape
    pairs = width // (3 * PAIR)

    def column(offset):
        return pl.BlockSpec((rows, PAIR), lambda h, info: (0, offset + h))

    shape = jax.ShapeDtypeStruct((rows, pairs * PAIR), LOW)
    return pl.pallas_call(
        functools.partial(attend_back_kernel, block),
        grid_spec=pltpu.PrefetchScalarGridSpec(
            num_scalar_prefetch=1,
            grid=(pairs,),
            in_specs=[column(0), column(pairs), column(2 * pairs), column(0), column(0), column(0)],
            out_specs=[column(0)] * 3,
            scratch_shapes=[
                pltpu.VMEM((block, PAIR), F32),
                pltpu.VMEM((rows, PAIR), F32),
                pltpu.VMEM((rows, PAIR), F32),
            ],
        ),
        out_shape=[shape] * 3,
        name="attend_back",
    )(info, qkv, qkv, qkv, grad_out, mixed, totals)


def after(value, *others):
    return lax.optimization_barrier((value,) + others)[0]


def layer(
    patches,
    lengths,
    deal,
    attn_gain,
    w_query,
    w_key,
    w_value,
    w_out,
    ffn_gain,
    w_gate,
    w_up,
    w_down,
    cotangent,
):
    groups = lax.axis_size("dp")
    seq_total = patches.shape[0]
    band = patches.shape[2]
    quarter = cotangent.shape[2]
    width = patches.shape[3]
    group = lax.axis_index("dp")
    place = lax.axis_index("tensor")
    chip = place // 2
    core = place % 2

    def swap_core(value):
        return lax.ppermute(value, "tensor", [(0, 1), (1, 0), (2, 3), (3, 2)])

    def swap_chip(value):
        return lax.ppermute(value, "tensor", [(0, 2), (2, 0), (1, 3), (3, 1)])

    def exchange(value):
        return lax.all_to_all(value, "dp", split_axis=0, concat_axis=0, tiled=True)

    slot_owner = jnp.argsort(deal)
    owners = slot_owner.reshape(groups, 2)
    mine = jnp.take(owners, chip, axis=1)
    theirs = jnp.take(owners, 1 - chip, axis=1)
    length = lengths[mine[group]]
    given = swap_chip(patches[theirs, 0])
    arrived_near = exchange(patches[mine, 0])
    arrived_far = exchange(given)
    inputs = jnp.stack((arrived_near, arrived_far)).reshape(2 * quarter, width).astype(F32)

    w_qkv = jnp.concatenate((w_query, w_key, w_value), 1)
    w_qkv_far = swap_chip(w_qkv)
    w_out_far = swap_chip(w_out)
    w_gate_far = swap_chip(w_gate)
    w_up_far = swap_chip(w_up)
    w_down_far = swap_chip(w_down)
    cot_near = jnp.take(cotangent[:, 0], chip, axis=0)
    cot_far = swap_chip(jnp.take(cotangent[:, 0], 1 - chip, axis=0))

    numbers = jnp.arange(4)
    slots = 2 * (numbers % 2 != core) + (numbers // 2 != chip)
    live_blocks = (length + quarter - 1) // quarter
    info = jnp.concatenate((live_blocks[None], slots)).astype(jnp.int32)
    offsets = jnp.arange(quarter)
    positions = jnp.concatenate(
        ((2 * chip + core) * quarter + offsets, (2 * (1 - chip) + core) * quarter + offsets)
    )
    live_rows = (positions < length).astype(F32)[:, None]
    own_rows = 2 * quarter

    def gather(value):
        other = swap_core(value)
        return jnp.concatenate((value, other), 0)

    def scatter(make):
        far = make(slice(own_rows, None)).astype(LOW)
        far = swap_core(far)
        return make(slice(0, own_rows)) + far.astype(F32)

    normed_attn, factor_attn = norm_rows(inputs, attn_gain)
    rows_attn = gather(normed_attn)
    qkv = [dot(rows_attn, w, 1, 0, LOW) for w in (w_qkv, w_qkv_far)]
    mixed_near, total_near = attend(info, qkv[0], quarter)
    mixed_far, total_far = attend(info, qkv[1], quarter)
    attention = scatter(
        lambda part: dot(mixed_near[part], w_out, 1, 0) + dot(mixed_far[part], w_out_far, 1, 0),
    )
    hidden = inputs + attention
    normed_ffn, factor_ffn = norm_rows(hidden, ffn_gain)
    rows_ffn = gather(normed_ffn)
    gates = jnp.concatenate((w_gate, w_gate_far), 1)
    ups = jnp.concatenate((w_up, w_up_far), 1)
    downs = jnp.concatenate((w_down, w_down_far), 0)
    gate_pre = dot(rows_ffn, gates, 1, 0, LOW).astype(F32)
    up_proj = dot(rows_ffn, ups, 1, 0, LOW).astype(F32)
    sigmoid = 1.0 / (1.0 + jnp.exp(-gate_pre))
    swish_gate = gate_pre * sigmoid
    product = (swish_gate * up_proj).astype(LOW)
    feedforward = scatter(lambda part: dot(product[part], downs, 1, 0))
    result = (live_rows * (hidden + feedforward)).astype(LOW)
    result_far = swap_chip(result[quarter:])
    output = jnp.where(
        chip == 0,
        jnp.stack((result[:quarter], result_far)),
        jnp.stack((result_far, result[:quarter])),
    )[:, None]

    grad_result = jnp.concatenate((cot_near, cot_far), 0).astype(F32) * live_rows
    grad_ffn = gather(grad_result.astype(LOW))
    grad_product = dot(grad_ffn, downs, 1, 1)
    grad_gate = (grad_product * up_proj * sigmoid * (1.0 + gate_pre * (1.0 - sigmoid))).astype(LOW)
    grad_up = (grad_product * swish_gate).astype(LOW)

    half = w_gate.shape[1]

    def over_chips(parts):
        far = swap_chip(jnp.concatenate([far.astype(LOW) for _, far in parts], 0))
        summed = jnp.concatenate([near for near, _ in parts], 0) + far.astype(F32)
        rows = summed.shape[0]
        held = summed.reshape(rows, groups, width // groups).transpose(1, 0, 2)
        step = 1
        while step < groups:
            side = (group // step) % 2
            pairs = held.reshape(-1, 2, rows, width // groups)
            moved = lax.ppermute(
                lax.dynamic_index_in_dim(pairs, 1 - side, 1, False).astype(LOW),
                "dp",
                [(i, i ^ step) for i in range(groups)],
            )
            held = lax.dynamic_index_in_dim(pairs, side, 1, False) + moved.astype(F32)
            step *= 2
        return held[0]

    def halves(value):
        return (value[:half], value[half:])

    down_shard = over_chips([halves(dot(product, grad_ffn, 0, 0))])
    up_halves = halves(dot(grad_up, rows_ffn, 0, 0))
    gate_up_shards = over_chips([halves(dot(grad_gate, rows_ffn, 0, 0)), up_halves])
    grad_normed_ffn = scatter(
        lambda part: dot(grad_gate[part], gates, 1, 1) + dot(grad_up[part], ups, 1, 1),
    )
    grad_hidden, gain_ffn_part = norm_back(hidden, factor_ffn, ffn_gain, grad_normed_ffn)
    grad_hidden = grad_hidden + grad_result
    grad_attn = gather(grad_hidden.astype(LOW))
    out_halves = (dot(mixed_near, grad_attn, 0, 0), dot(mixed_far, grad_attn, 0, 0))
    back_far = dot(grad_attn, w_out_far, 1, 1, LOW)
    grad_far = attend_back(info, qkv[1], back_far, mixed_far, total_far, quarter)
    grad_far = jnp.concatenate(grad_far, 1)
    weight_far = dot(grad_far, rows_attn, 0, 0, LOW)
    back_near = after(dot(grad_attn, w_out, 1, 1, LOW), weight_far)
    grad_near = attend_back(info, qkv[0], back_near, mixed_near, total_near, quarter)
    grad_near = jnp.concatenate(grad_near, 1)
    grad_normed_attn = scatter(
        lambda part: dot(grad_near[part], w_qkv, 1, 1) + dot(grad_far[part], w_qkv_far, 1, 1),
    )
    qkv_shards = over_chips([out_halves, (dot(grad_near, rows_attn, 0, 0), weight_far)])
    grad_inputs, gain_attn_part = norm_back(inputs, factor_attn, attn_gain, grad_normed_attn)
    grad_inputs = (grad_inputs + grad_hidden).astype(LOW)
    returned = exchange(grad_inputs[quarter:].reshape(groups, band, width))
    by_far = swap_chip(returned)
    by_near = exchange(grad_inputs[:quarter].reshape(groups, band, width))
    by_slot = jnp.where(
        chip == 0, jnp.stack((by_near, by_far), 1), jnp.stack((by_far, by_near), 1)
    ).reshape(seq_total, band, width)
    grad_patches = by_slot[deal][:, None]

    def total_of(value):
        value = value + swap_core(value)
        value = value + swap_chip(value)
        step = 1
        while step < groups:
            moved = lax.ppermute(value, "dp", [(i, i ^ step) for i in range(groups)])
            value = value + moved
            step *= 2
        return value

    gain_grads = total_of(jnp.stack((gain_attn_part, gain_ffn_part)))
    part = w_query.shape[1]
    return (
        output,
        grad_patches,
        gain_grads[0],
        qkv_shards[part : 2 * part].T,
        qkv_shards[2 * part : 3 * part].T,
        qkv_shards[3 * part :].T,
        qkv_shards[:part],
        gain_grads[1],
        gate_up_shards[:half].T,
        gate_up_shards[half:].T,
        down_shard,
    )


def solution(mesh):
    in_specs = (
        P(None, "tensor", "dp", None),
        P(),
        P(),
        P(),
        P(None, "tensor"),
        P(None, "tensor"),
        P(None, "tensor"),
        P("tensor", None),
        P(),
        P(None, "tensor"),
        P(None, "tensor"),
        P("tensor", None),
        P("dp", "tensor", None, None),
    )
    out_specs = (
        P("dp", "tensor", None, None),
        P(None, "tensor", "dp", None),
        P(),
        P("dp", "tensor"),
        P("dp", "tensor"),
        P("dp", "tensor"),
        P("tensor", "dp"),
        P(),
        P("dp", "tensor"),
        P("dp", "tensor"),
        P("tensor", "dp"),
    )
    return jax.shard_map(layer, mesh=mesh, in_specs=in_specs, out_specs=out_specs, check_vma=False)
```
